256 devices in a mesh: dom: 64 (over z, y, core), rep: 4 (over x).
Axes of the slice: x: 4, y: 4, z: 8, core: 2. Of those that a mesh axis runs over, the one named last changes fastest.
Arguments:
- ns_shape: bfloat16 [64, 256], replicated, may hold values from -0.75 to 0.75
- nm_shape: bfloat16 [64, 256], replicated, may hold values from -0.75 to 0.75
- sec_disp: bfloat16 [64, 2097152], P(None, ('dom', 'rep')), may hold values from -6 to 6
- mst_disp: bfloat16 [64, 2097152], P(None, ('dom', 'rep')), may hold values from -6 to 6
- gap_offset: float32 [2097152], P(('dom', 'rep')), may hold values from -6 to 6
- quad_weight: float32 [256], replicated, may hold values from 0.25 to 4
- jacobian: float32 [2097152], P(('dom', 'rep')), may hold values from 0.0005 to 0.005
- segment_slot: int32 [2097152], P(('dom', 'rep')), may hold values from 0 to 1279, as said below
- face_id: int32 [2097152], P(('dom', 'rep')), may hold values from 0 to 1073741823
- search_rank: int32 [2097152], P(('dom', 'rep')), may hold values from 0 to 3
- live_rows: int32 [256], P(('dom', 'rep')), may hold values from 1024 to 8192, as said below
Outputs:
- contact_force: bfloat16 [64, 2097152], P(None, ('dom', 'rep'))
- seg_pen: float32 [65536], P('dom')
- seg_face: int32 [65536], P('dom')
- seg_gap: float32 [65536], P('dom')
- mean_gap: float32 [], replicated
The draws below stay inside these ranges and needn't reach their ends.
Inputs may be any that keep to these rules, and one draw needn't show every extreme that they name: `segment_slot`: A row's segment is (1024 times the dom index of its device plus its slot) modulo 65536; slots of 1024 or more reach the next dom index's first 256 segments. `live_rows`: entry b counts the live rows of the device with flat index b (dom-major); they are that device's first rows, the rest are padding; some device is full in every draw.
All inputs are finite; a program needn't handle non-finite values.
Results may differ from the reference program's by a relative error of at most 0.0055.
Values sent between devices are 32-bit elements; how exact they have to be, the bound alone decides.
A program may use at most 64 MiB of HBM per device.

```python
import math
import jax
import jax.numpy as jnp
from jax import lax

P_SIZE = 256
K = 64
ROWS_DEV = 8192
SEG_DEV = 1024
SPILL = 256
SEGS = 65536
ROWS = 2097152
N_REP = 4
DEVICES = 256


def draw_live_rows(key, part):
    first_key = jax.random.fold_in(key, 11)
    second_key = jax.random.fold_in(key, 23)
    counts = jax.random.randint(first_key, (DEVICES,), ROWS_DEV // 8, ROWS_DEV + 1, dtype=jnp.int32)
    full_device = jax.random.randint(second_key, (), 0, DEVICES, dtype=jnp.int32)
    return jnp.where(jnp.arange(DEVICES, dtype=jnp.int32) == full_device, ROWS_DEV, counts).astype(jnp.int32)


def draw_segment_slot(key, part):
    window_len = SEG_DEV + SPILL
    dom_count = DEVICES // N_REP
    vacant = jax.random.randint(jax.random.fold_in(key, 31), (SEGS,), 0, 8, dtype=jnp.int32) == 0
    forced = jax.random.randint(jax.random.fold_in(key, 37), (), 0, SEGS, dtype=jnp.int32)
    vacant = vacant | (jnp.arange(SEGS, dtype=jnp.int32) == forced)
    dom_ids = jnp.arange(dom_count, dtype=jnp.int32)
    window_ids = ((dom_ids[:, None] * SEG_DEV + jnp.arange(window_len, dtype=jnp.int32)[None, :]) % SEGS).astype(jnp.int32)
    blocked = vacant[window_ids].astype(jnp.int32)
    order = jnp.argsort(blocked, axis=1, stable=True).astype(jnp.int32)
    allowed = jnp.maximum(window_len - jnp.sum(blocked, axis=1), 1).astype(jnp.int32)
    row_dom = (jnp.arange(ROWS, dtype=jnp.int32) // (ROWS_DEV * N_REP)).astype(jnp.int32)
    raw_pick = jax.random.randint(jax.random.fold_in(key, 41), (ROWS,), 0, 1 << 24, dtype=jnp.int32)
    pick = (raw_pick % allowed[row_dom]).astype(jnp.int32)
    return order[row_dom, pick].astype(jnp.int32)


def set_ends(drawn, own_key, least, top_value):
    longest = drawn.shape.index(max(drawn.shape))
    spots = []
    for shift in (0, 1):
        where = [jax.random.randint(jax.random.fold_in(own_key, axis), (), 0, length) for axis, length in enumerate(drawn.shape)]
        where[longest] = (where[longest] + shift) % drawn.shape[longest]
        spots.append(tuple(where))
    return drawn.at[spots[0]].set(least).at[spots[1]].set(top_value)


def levels(stream_key, extent, cuts, least, high):
    level, own = 1.0, jax.random.fold_in(stream_key, 6)
    for dim, shards_of in cuts:
        steps = jnp.exp(jax.random.uniform(jax.random.fold_in(own, dim), (shards_of,), jnp.float32, least / len(cuts), high / len(cuts)))
        level = level * jnp.repeat(steps, extent[dim] // shards_of).reshape([-1 if axis == dim else 1 for axis in range(len(extent))])
    return level


def centred(key, extent, scale, most, pieces=(), held_as=jnp.bfloat16):
    result = scale * jax.random.normal(key, extent, jnp.float32)
    if pieces:
        result = result * levels(key, extent, pieces, -0.22, 0.18)
    return jnp.clip(result, -most, most).astype(held_as)


def setup_inputs(seed: int = 0) -> dict:
    key_of = jax.random.split(jax.random.key(seed), 12)
    return {
        "ns_shape": centred(key_of[0], (K, P_SIZE), K ** -0.5, 0.75),
        "nm_shape": centred(key_of[1], (K, P_SIZE), K ** -0.5, 0.75),
        "sec_disp": centred(key_of[2], (K, ROWS), 1.0, 6.0, ((1, 256),)),
        "mst_disp": centred(key_of[3], (K, ROWS), 1.0, 6.0, ((1, 256),)),
        "gap_offset": centred(key_of[4], (ROWS,), 1.0, 6.0, ((0, 256),), jnp.float32),
        "quad_weight": jnp.clip(jnp.exp(jax.random.uniform(key_of[5], (P_SIZE,), jnp.float32, math.log(0.25), math.log(4.0))), 0.25, 4.0),
        "jacobian": jnp.clip(jnp.exp(math.log(0.005) - 2.30258502 * jax.random.uniform(key_of[6], (ROWS,), jnp.float32) ** levels(key_of[6], (ROWS,), ((0, 256),), -0.2, 0.2)), 0.0005, 0.005),
        "segment_slot": draw_segment_slot(jax.random.fold_in(key_of[11], 71), 0),
        "face_id": set_ends(jax.random.randint(key_of[8], (ROWS,), 0, 1073741824), jax.random.fold_in(key_of[8], 1), 0, 1073741823).astype(jnp.int32),
        "search_rank": set_ends(jax.random.randint(key_of[9], (ROWS,), 0, 4), jax.random.fold_in(key_of[9], 1), 0, 3).astype(jnp.int32),
        "live_rows": draw_live_rows(jax.random.fold_in(key_of[11], 71), 0),
    }


PENALTY = 400.0
LOWEST_FILL = -1.0e30
FACE_LIMIT = 1073741824


def project(shape_table, displace):
    return lax.dot_general(shape_table, displace, (((0,), (0,)), ((), ())), preferred_element_type=jnp.float32)


def window_stats(gap_field, jac_row, weights, slots, faces, ranks, live, window_len):
    row_pen = jnp.max(-gap_field, axis=0)
    row_gap = jac_row * jnp.dot(weights, gap_field, precision=lax.Precision.HIGHEST)
    row_area = jac_row * jnp.sum(weights)
    penalty_max = jnp.maximum(jax.ops.segment_max(jnp.where(live, row_pen, LOWEST_FILL), slots, num_segments=window_len), LOWEST_FILL)
    best_rank = jnp.maximum(jax.ops.segment_max(jnp.where(live, ranks, -1), slots, num_segments=window_len), -1).astype(jnp.int32)
    chosen = jnp.where(live & (ranks == best_rank[slots]), faces, FACE_LIMIT).astype(jnp.int32)
    lowest_face = jnp.minimum(jax.ops.segment_min(chosen, slots, num_segments=window_len), FACE_LIMIT).astype(jnp.int32)
    gap_sum = jax.ops.segment_sum(jnp.where(live, row_gap, 0.0), slots, num_segments=window_len)
    area_sum = jax.ops.segment_sum(jnp.where(live, row_area, 0.0), slots, num_segments=window_len)
    return penalty_max, best_rank, lowest_face, gap_sum, area_sum


def reference(ns_shape, nm_shape, sec_disp, mst_disp, gap_offset, quad_weight, jacobian, segment_slot, face_id, search_rank, live_rows):
    row_count = ROWS_DEV
    window_len = SEG_DEV + SPILL

    def blocks(values):
        return values.reshape(DEVICES, row_count)

    sec_blocks = sec_disp.reshape(K, DEVICES, row_count).transpose(1, 0, 2)
    mst_blocks = mst_disp.reshape(K, DEVICES, row_count).transpose(1, 0, 2)

    def one_block(block):
        sec_part, mst_part, offset, jac_row, slots, faces, ranks, live_count = block
        gap_field = project(ns_shape, sec_part) - project(nm_shape, mst_part) + offset[None, :]
        live = jnp.arange(row_count, dtype=jnp.int32) < live_count
        load = jnp.where(live[None, :], quad_weight[:, None] * jac_row[None, :] * PENALTY * jnp.maximum(-gap_field, 0.0), 0.0).astype(jnp.bfloat16)
        force = jnp.dot(ns_shape, load, preferred_element_type=jnp.float32).astype(jnp.bfloat16)
        stats = window_stats(gap_field, jac_row, quad_weight, slots, faces, ranks, live, window_len)
        return (force,) + stats

    outputs = lax.map(one_block, (sec_blocks, mst_blocks, blocks(gap_offset), blocks(jacobian), blocks(segment_slot), blocks(face_id), blocks(search_rank), live_rows))
    force_blocks, penalty_max, best_rank, lowest_face, gap_sum, area_sum = outputs
    contact_force = force_blocks.transpose(1, 0, 2).reshape(K, DEVICES * row_count)
    dom_index = (jnp.arange(DEVICES, dtype=jnp.int32) // N_REP).astype(jnp.int32)
    seg_ids = ((dom_index[:, None] * SEG_DEV + jnp.arange(window_len, dtype=jnp.int32)[None, :]) % SEGS).astype(jnp.int32).reshape(-1)
    seg_max = jnp.maximum(jax.ops.segment_max(penalty_max.reshape(-1), seg_ids, num_segments=SEGS), LOWEST_FILL)
    seg_rank = jnp.maximum(jax.ops.segment_max(best_rank.reshape(-1), seg_ids, num_segments=SEGS), -1).astype(jnp.int32)
    chosen = jnp.where(best_rank.reshape(-1) == seg_rank[seg_ids], lowest_face.reshape(-1), FACE_LIMIT).astype(jnp.int32)
    seg_low = jnp.minimum(jax.ops.segment_min(chosen, seg_ids, num_segments=SEGS), FACE_LIMIT).astype(jnp.int32)
    seg_pen = jnp.where(seg_rank < 0, jnp.float32(0.0), seg_max)
    seg_face = jnp.where(seg_rank < 0, -1, seg_low).astype(jnp.int32)
    seg_gap = jax.ops.segment_sum(gap_sum.reshape(-1), seg_ids, num_segments=SEGS)
    mean_gap = jnp.sum(gap_sum) / jnp.sum(area_sum)
    return contact_force, seg_pen, seg_face, seg_gap, mean_gap
```

```python
import jax
import jax.numpy as jnp
from jax import lax
from jax.experimental import pallas as pl
from jax.experimental.pallas import tpu as pltpu
from jax.sharding import Mesh
from jax.sharding import PartitionSpec as P

SEG_DEV = 1024
SPILL = 256
P_SIZE = 256
K = 64
LANES = 128
HIS = 10
DOM = ("dom_0", "dom_1", "dom_2")
DOM_REP = ("dom_0", "dom_1", "dom_2", "rep")
PENALTY = 400.0
LOWEST_FILL = -1e30
FACE_LIMIT = 1073741824
KEY_LOW = -2147483648
CHUNK = 1024
F32 = jnp.float32
BF16 = jnp.bfloat16


def pieces(x):
    high = x.astype(BF16)
    rest = x - high.astype(F32)
    mid = rest.astype(BF16)
    low = (rest - mid.astype(F32)).astype(BF16)
    return high.astype(F32), mid.astype(F32), low.astype(F32)


def fold_rows(x, op):
    while x.shape[0] > 8:
        half = x.shape[0] // 2
        x = op(x[:half], x[half:])
    for shift in (4, 2, 1):
        x = op(x, pltpu.roll(x, shift, 0))
    return x


def local_kernel(
    ns_ref, nm_ref, sec_hbm, mst_hbm, off_ref, qw_ref, jac_ref, slot_ref, face_ref, rank_ref, live_ref,
    force_hbm, pen_ref, rank_out, face_out, gap_ref, area_ref,
    sec_buf, mst_buf, force_buf, table, weight, pen_by, key_by, lo_ref, acc_pen, acc_key, in_sem, out_sem,
):
    rows = sec_hbm.shape[1]
    chunks = rows // CHUNK

    def load(c):
        part = pl.ds(c * CHUNK, CHUNK)
        return (
            pltpu.make_async_copy(sec_hbm.at[:, part], sec_buf.at[:, part], in_sem.at[0, c]),
            pltpu.make_async_copy(mst_hbm.at[:, part], mst_buf.at[:, part], in_sem.at[1, c]),
        )

    def save(c):
        part = pl.ds(c * CHUNK, CHUNK)
        return pltpu.make_async_copy(force_buf.at[:, part], force_hbm.at[:, part], out_sem.at[c])

    for c in range(chunks):
        for copy in load(c):
            copy.start()

    ns = ns_ref[...]
    both = jnp.concatenate([ns.astype(F32), -nm_ref[...].astype(F32)], axis=0).T
    column = jnp.broadcast_to(qw_ref[...], (LANES, P_SIZE)).T
    weight[...] = column * (-PENALTY)
    total_weight = jnp.sum(qw_ref[...], axis=1, keepdims=True)
    coefficient = jnp.sum(both * column, axis=0, keepdims=True)
    high, mid, low = pieces(coefficient)
    eight = lax.broadcasted_iota(jnp.int32, (8, LANES), 0)
    extra = jnp.where(eight == 0, high, jnp.where(eight == 1, mid, jnp.where(eight == 2, low, 0.0)))
    lane = lax.broadcasted_iota(jnp.int32, (P_SIZE + 16, LANES), 1)
    row = lax.broadcasted_iota(jnp.int32, (P_SIZE + 16, LANES), 0)
    table[:, :LANES] = jnp.concatenate([both, extra, jnp.zeros_like(extra)], axis=0).astype(BF16)
    table[:, LANES:] = jnp.where((lane < 3) & (row < P_SIZE), 1.0, 0.0).astype(BF16)

    live_count = live_ref[0]
    sums = jnp.zeros((48, LANES), F32)
    area = jnp.zeros((1, CHUNK), F32)
    for c in range(chunks):
        part = pl.ds(c * CHUNK, CHUNK)
        offset, jacobian = off_ref[:, part], jac_ref[:, part]
        slots = slot_ref[:, part]
        live = lax.broadcasted_iota(jnp.int32, (1, CHUNK), 1) < live_count - c * CHUNK
        for copy in load(c):
            copy.wait()
        o_high, o_mid, o_low = pieces(offset)
        sixteen = lax.broadcasted_iota(jnp.int32, (16, CHUNK), 0)
        tail = jnp.where(
            sixteen == 0, o_high, jnp.where(sixteen == 1, o_mid, jnp.where(sixteen == 2, o_low, 0.0))
        ).astype(BF16)
        data = jnp.concatenate([sec_buf[:, part], mst_buf[:, part], tail], axis=0)
        found = jnp.dot(table[:, :144], data, preferred_element_type=F32)
        gap = found[:P_SIZE]
        row_pen = -jnp.min(gap, axis=0, keepdims=True)
        row_gap = jacobian * (
            found[P_SIZE : P_SIZE + 1]
            + found[P_SIZE + 1 : P_SIZE + 2]
            + found[P_SIZE + 2 : P_SIZE + 3]
            + offset * total_weight
        )
        column_weight = jnp.tile(weight[...], (1, CHUNK // LANES))
        load_field = (jnp.maximum(column_weight * gap, 0.0) * jnp.where(live, jacobian, 0.0)).astype(BF16)
        force_buf[:, part] = jnp.dot(ns, load_field, preferred_element_type=F32).astype(BF16)
        save(c).start()

        area = area + jnp.where(live, jacobian, 0.0)
        hi = jnp.where(live, lax.shift_right_logical(slots, 7), 99)
        lo = slots & (LANES - 1)
        member = sixteen == hi
        key = (rank_ref[:, part] - 2) * FACE_LIMIT + (FACE_LIMIT - 1 - face_ref[:, part])
        pens = jnp.where(member, row_pen, LOWEST_FILL)
        keys = jnp.where(member, key, KEY_LOW)
        for j in range(CHUNK // LANES):
            at = slice(j * LANES, (j + 1) * LANES)
            pen_by[c * (CHUNK // LANES) + j] = pens[:, at]
            key_by[c * (CHUNK // LANES) + j] = keys[:, at]
            lo_ref[c * (CHUNK // LANES) + j] = jnp.broadcast_to(lo[:, at], (8, LANES))
        split = jnp.concatenate([jnp.where(member, piece, 0.0) for piece in pieces(row_gap)], axis=0)
        ids = lax.broadcasted_iota(jnp.int32, (LANES, CHUNK), 0)
        one_hot = jnp.where(ids == lo, 1.0, 0.0).astype(BF16)
        sums = sums + lax.dot_general(
            split.astype(BF16), one_hot, (((1,), (1,)), ((), ())), preferred_element_type=F32
        )
    gap_ref[...] = sums[:16] + sums[16:32] + sums[32:]
    area_ref[...] = jnp.broadcast_to(jnp.sum(area, axis=1, keepdims=True) * total_weight, (8, LANES))

    group = 2
    for g in range(LANES // (8 * group)):
        ids = [eight + 8 * (g * group + j) for j in range(group)]

        def step(i, carry):
            pens, keys = carry
            lo = lo_ref[i]
            masks = [lo == ids[j] for j in range(group)]
            new_pens, new_keys = [], []
            for h in range(HIS):
                pen = pen_by[i, pl.ds(h, 8, stride=0), :]
                key = key_by[i, pl.ds(h, 8, stride=0), :]
                for j in range(group):
                    k = h * group + j
                    new_pens.append(jnp.maximum(pens[k], jnp.where(masks[j], pen, LOWEST_FILL)))
                    new_keys.append(jnp.maximum(keys[k], jnp.where(masks[j], key, KEY_LOW)))
            return new_pens, new_keys

        start = (
            [jnp.full((8, LANES), LOWEST_FILL, F32)] * (HIS * group),
            [jnp.full((8, LANES), KEY_LOW, jnp.int32)] * (HIS * group),
        )
        pens, keys = lax.fori_loop(0, rows // LANES, step, start, unroll=2)
        for h in range(HIS):
            for j in range(group):
                at = pl.ds(8 * (g * group + j), 8)
                acc_pen[h, at, :] = pens[h * group + j]
                acc_key[h, at, :] = keys[h * group + j]

    for h in range(HIS):
        pen = fold_rows(acc_pen[h].T, jnp.maximum)[:1]
        key = fold_rows(acc_key[h].T, jnp.maximum)[:1]
        empty = pen <= 0.5 * LOWEST_FILL
        pen_ref[h : h + 1, :] = pen
        rank_out[h : h + 1, :] = jnp.where(empty, -1, lax.shift_right_arithmetic(key, 30) + 2)
        face_out[h : h + 1, :] = jnp.where(empty, FACE_LIMIT, FACE_LIMIT - 1 - (key & (FACE_LIMIT - 1)))
    for c in range(chunks):
        save(c).wait()


def local_part(ns, nm, sec, mst, off, qw, jac, slot, face, rank, live):
    rows = sec.shape[1]
    chunks = rows // CHUNK
    vmem = pl.BlockSpec(memory_space=pltpu.VMEM)
    hbm = pl.BlockSpec(memory_space=pl.ANY)
    smem = pl.BlockSpec(memory_space=pltpu.SMEM)
    line = lambda x: x.reshape(1, -1)
    return pl.pallas_call(
        local_kernel,
        out_shape=(
            jax.ShapeDtypeStruct((K, rows), BF16),
            jax.ShapeDtypeStruct((16, LANES), F32),
            jax.ShapeDtypeStruct((16, LANES), jnp.int32),
            jax.ShapeDtypeStruct((16, LANES), jnp.int32),
            jax.ShapeDtypeStruct((16, LANES), F32),
            jax.ShapeDtypeStruct((8, LANES), F32),
        ),
        in_specs=[vmem, vmem, hbm, hbm, vmem, vmem, vmem, vmem, vmem, vmem, smem],
        out_specs=(hbm, vmem, vmem, vmem, vmem, vmem),
        scratch_shapes=[
            pltpu.VMEM((K, rows), BF16),
            pltpu.VMEM((K, rows), BF16),
            pltpu.VMEM((K, rows), BF16),
            pltpu.VMEM((P_SIZE + 16, 2 * LANES), BF16),
            pltpu.VMEM((P_SIZE, LANES), F32),
            pltpu.VMEM((rows // LANES, 16, LANES), F32),
            pltpu.VMEM((rows // LANES, 16, LANES), jnp.int32),
            pltpu.VMEM((rows // LANES, 8, LANES), jnp.int32),
            pltpu.VMEM((HIS, LANES, LANES), F32),
            pltpu.VMEM((HIS, LANES, LANES), jnp.int32),
            pltpu.SemaphoreType.DMA((2, chunks)),
            pltpu.SemaphoreType.DMA((chunks,)),
        ],
        compiler_params=pltpu.CompilerParams(vmem_limit_bytes=48 << 20),
    )(ns, nm, sec, mst, line(off), line(qw), line(jac), line(slot), line(face), line(rank), live)


def combine(earlier, latter):
    prefer = (latter[1] > earlier[1]) | (latter[1] == earlier[1]) & (latter[2] < earlier[2])
    return (
        jnp.maximum(earlier[0], latter[0]),
        jnp.where(prefer, latter[1], earlier[1]),
        jnp.where(prefer, latter[2], earlier[2]),
        earlier[3] + latter[3],
    )


def shards(*args):
    force, pen, rank, face, gap, area = local_part(*args)
    stats = (pen[:HIS], rank[:HIS], face[:HIS], gap[:HIS])
    length = lax.axis_size(DOM)
    moved = [(i, (i + 1) % length) for i in range(length)]
    incoming = [lax.ppermute(part[8:], DOM, moved) for part in stats]
    leading = combine([part[:2] for part in stats], incoming)
    owned = [jnp.concatenate([a, b[2:8]]) for a, b in zip(leading, stats)]
    shared = [lax.all_gather(part, "rep") for part in owned]
    own = [part[0] for part in shared]
    for k in range(1, 4):
        own = combine(own, [part[k] for part in shared])
    empty = own[1] < 0
    seg_pen = jnp.where(empty, 0.0, own[0]).reshape(-1)
    seg_face = jnp.where(empty, -1, own[2]).reshape(-1)
    totals = lax.psum((jnp.sum(gap), area[0, 0]), DOM_REP)
    return force, seg_pen, seg_face, own[3].reshape(-1), totals[0] / totals[1]


def solution(mesh):
    finer = Mesh(mesh.devices.reshape(8, 4, 2, mesh.shape["rep"]), DOM_REP)
    placed = (P(), P(), P(None, DOM_REP), P(None, DOM_REP), P(DOM_REP), P()) + (P(DOM_REP),) * 5
    return jax.shard_map(
        shards,
        mesh=finer,
        in_specs=placed,
        out_specs=(P(None, DOM_REP), P(DOM), P(DOM), P(DOM), P()),
        check_vma=False,
    )
```

```python
import jax
import jax.numpy as jnp
from jax import lax
from jax.experimental import pallas as pl
from jax.experimental.pallas import tpu as pltpu
from jax.sharding import PartitionSpec as P

P_SIZE = 256
K = 64
LANES = 128
HIS = 10
PENALTY = 400.0
LOWEST_FILL = -1e30
FACE_LIMIT = 1073741824
KEY_LOW = -2147483648
CHUNK = 1024
F32 = jnp.float32
I32 = jnp.int32
BF16 = jnp.bfloat16
MESH = pl.DeviceIdType.MESH
DOMS = 64
REPS = 4
PLANE_DOMS = 8
PLANE = PLANE_DOMS * REPS
LAYERS = DOMS // PLANE_DOMS
GREETED = PLANE - 1 + LAYERS - 1 + REPS


def pieces(x):
    high = x.astype(BF16)
    rest = x - high.astype(F32)
    mid = rest.astype(BF16)
    low = (rest - mid.astype(F32)).astype(BF16)
    return high.astype(F32), mid.astype(F32), low.astype(F32)


def fold_rows(x, op):
    while x.shape[0] > 8:
        half = x.shape[0] // 2
        x = op(x[:half], x[half:])
    for shift in (4, 2, 1):
        x = op(x, pltpu.roll(x, shift, 0))
    return x


def combine(earlier, latter):
    prefer = (latter[1] > earlier[1]) | (latter[1] == earlier[1]) & (latter[2] < earlier[2])
    return (
        jnp.maximum(earlier[0], latter[0]),
        jnp.where(prefer, latter[1], earlier[1]),
        jnp.where(prefer, latter[2], earlier[2]),
        earlier[3] + latter[3],
    )


def kernel(
    ns_hbm, nm_hbm, sec_hbm, mst_hbm, off_hbm, qw_hbm, jac_hbm, slot_hbm, face_hbm, rank_hbm, live_ref,
    force_hbm, pen_out, face_out, gap_out, mean_out,
    ns_buf, nm_buf, sec_buf, mst_buf, off_buf, qw_buf, jac_buf, slot_buf, face_buf, rank_buf,
    force_buf, loads, table, weight, pen_by, key_by, lo_by, acc_pen, acc_key,
    plane_box, layer_box, own_f, own_i, spill_f, spill_i, got_f, got_i,
    in_sem, out_sem, plane_sem, layer_sem, own_sem, spill_sem,
):
    rows = sec_hbm.shape[1]
    chunks = rows // CHUNK
    dom, rep = lax.axis_index("dom"), lax.axis_index("rep")
    layer, spot = dom // PLANE_DOMS, (dom % PLANE_DOMS) * REPS + rep

    def plane_device(k):
        other = (spot + k) % PLANE
        return layer * PLANE_DOMS + other // REPS, other % REPS

    def layer_device(k):
        return (layer + k) % LAYERS * PLANE_DOMS + dom % PLANE_DOMS, rep

    barrier = pltpu.get_barrier_semaphore()

    def greet(device):
        pl.semaphore_signal(barrier, inc=1, device_id=device, device_id_type=MESH)

    def load(c):
        part = pl.ds(c * CHUNK, CHUNK)
        return (
            pltpu.make_async_copy(sec_hbm.at[:, part], sec_buf.at[:, part], in_sem.at[c]),
            pltpu.make_async_copy(mst_hbm.at[:, part], mst_buf.at[:, part], in_sem.at[chunks + c]),
        )

    whole = (
        (ns_hbm, ns_buf), (nm_hbm, nm_buf), (qw_hbm, qw_buf), (off_hbm, off_buf), (jac_hbm, jac_buf),
        (slot_hbm, slot_buf), (face_hbm, face_buf), (rank_hbm, rank_buf),
    )
    singles = [pltpu.make_async_copy(a, b, in_sem.at[2 * chunks + k]) for k, (a, b) in enumerate(whole)]
    for copy in singles[:3]:
        copy.start()
    for copy in load(0):
        copy.start()
    for copy in singles[3:]:
        copy.start()
    for c in range(1, chunks):
        for copy in load(c):
            copy.start()

    @pl.loop(1, PLANE)
    def _(k):
        greet(plane_device(k))

    @pl.loop(1, LAYERS)
    def _(k):
        greet(layer_device(k))

    @pl.loop(0, REPS)
    def _(k):
        greet(((dom + DOMS - 1) % DOMS, k))

    for copy in singles[:3]:
        copy.wait()
    ns = ns_buf[...]
    both = jnp.concatenate([ns.astype(F32), -nm_buf[...].astype(F32)], axis=0).T
    column = jnp.broadcast_to(qw_buf[...], (LANES, P_SIZE)).T
    weight[...] = column * (-PENALTY)
    total_weight = jnp.sum(qw_buf[...], axis=1, keepdims=True)
    coefficient = jnp.sum(both * column, axis=0, keepdims=True)
    high, mid, low = pieces(coefficient)
    eight = lax.broadcasted_iota(I32, (8, LANES), 0)
    extra = jnp.where(eight == 0, high, jnp.where(eight == 1, mid, jnp.where(eight == 2, low, 0.0)))
    lane = lax.broadcasted_iota(I32, (P_SIZE + 16, LANES), 1)
    row = lax.broadcasted_iota(I32, (P_SIZE + 16, LANES), 0)
    table[:, :LANES] = jnp.concatenate([both, extra, jnp.zeros_like(extra)], axis=0).astype(BF16)
    table[:, LANES:] = jnp.where((lane < 3) & (row < P_SIZE), 1.0, 0.0).astype(BF16)
    for copy in singles[3:]:
        copy.wait()

    live_count = live_ref[0]
    sums = jnp.zeros((48, LANES), F32)
    area = jnp.zeros((1, CHUNK), F32)
    for c in range(chunks):
        part = pl.ds(c * CHUNK, CHUNK)
        offset, jacobian = off_buf[:, part], jac_buf[:, part]
        slots = slot_buf[:, part]
        live = lax.broadcasted_iota(I32, (1, CHUNK), 1) < live_count - c * CHUNK
        for copy in load(c):
            copy.wait()
        o_high, o_mid, o_low = pieces(offset)
        sixteen = lax.broadcasted_iota(I32, (16, CHUNK), 0)
        tail = jnp.where(
            sixteen == 0, o_high, jnp.where(sixteen == 1, o_mid, jnp.where(sixteen == 2, o_low, 0.0))
        ).astype(BF16)
        data = jnp.concatenate([sec_buf[:, part], mst_buf[:, part], tail], axis=0)
        found = jnp.dot(table[:, :144], data, preferred_element_type=F32)
        gap = found[:P_SIZE]
        row_pen = -jnp.min(gap, axis=0, keepdims=True)
        row_gap = jacobian * (
            found[P_SIZE : P_SIZE + 1]
            + found[P_SIZE + 1 : P_SIZE + 2]
            + found[P_SIZE + 2 : P_SIZE + 3]
            + offset * total_weight
        )
        live_jacobian = jnp.where(live, jacobian, 0.0)
        column_weight = jnp.tile(weight[...], (1, CHUNK // LANES))
        loads[:, part] = (jnp.maximum(column_weight * gap, 0.0) * live_jacobian).astype(BF16)

        area = area + live_jacobian
        hi = jnp.where(live, lax.shift_right_logical(slots, 7), 99)
        lo = slots & (LANES - 1)
        member = sixteen == hi
        key = (rank_buf[:, part] - 2) * FACE_LIMIT + (FACE_LIMIT - 1 - face_buf[:, part])
        pens = jnp.where(member, row_pen, LOWEST_FILL)
        keys = jnp.where(member, key, KEY_LOW)
        for j in range(CHUNK // LANES):
            at = slice(j * LANES, (j + 1) * LANES)
            pen_by[c * (CHUNK // LANES) + j] = pens[:, at]
            key_by[c * (CHUNK // LANES) + j] = keys[:, at]
            lo_by[c * (CHUNK // LANES) + j] = jnp.broadcast_to(lo[:, at], (8, LANES))
        split = jnp.concatenate([jnp.where(member, piece, 0.0) for piece in pieces(row_gap)], axis=0)
        ids = lax.broadcasted_iota(I32, (LANES, CHUNK), 0)
        one_hot = jnp.where(ids == lo, 1.0, 0.0).astype(BF16)
        sums = sums + lax.dot_general(
            split.astype(BF16), one_hot, (((1,), (1,)), ((), ())), preferred_element_type=F32
        )
    seg_gap = sums[:16] + sums[16:32] + sums[32:]
    gap_total = jnp.sum(jnp.sum(seg_gap, axis=0, keepdims=True), axis=1, keepdims=True)
    area_total = jnp.sum(area, axis=1, keepdims=True) * total_weight
    first_lane = lax.broadcasted_iota(I32, (1, LANES), 1) == 0
    plane_box[spot] = jnp.where(first_lane, gap_total, area_total)

    def plane_copy(k):
        return pltpu.make_async_remote_copy(
            src_ref=plane_box.at[spot], dst_ref=plane_box.at[spot],
            send_sem=plane_sem.at[0, k], recv_sem=plane_sem.at[1, k],
            device_id=plane_device(k), device_id_type=MESH,
        )

    def layer_copy(k):
        return pltpu.make_async_remote_copy(
            src_ref=layer_box.at[layer], dst_ref=layer_box.at[layer],
            send_sem=layer_sem.at[0, k], recv_sem=layer_sem.at[1, k],
            device_id=layer_device(k), device_id_type=MESH,
        )

    pl.semaphore_wait(barrier, GREETED)

    @pl.loop(1, PLANE)
    def _(k):
        plane_copy(k).start()

    def best(first, last):
        @pl.loop(first, last)
        def _(g):
            base = pl.multiple_of(g * 8, 8)
            ids = eight + base

            def step(i, carry):
                pens, keys = carry
                mask = lo_by[i] == ids
                new_pens, new_keys = [], []
                for h in range(HIS):
                    pen = pen_by[i, pl.ds(h, 8, stride=0), :]
                    key = key_by[i, pl.ds(h, 8, stride=0), :]
                    new_pens.append(jnp.maximum(pens[h], jnp.where(mask, pen, LOWEST_FILL)))
                    new_keys.append(jnp.maximum(keys[h], jnp.where(mask, key, KEY_LOW)))
                return new_pens, new_keys

            start = (
                [jnp.full((8, LANES), LOWEST_FILL, F32)] * HIS,
                [jnp.full((8, LANES), KEY_LOW, I32)] * HIS,
            )
            pens, keys = lax.fori_loop(0, rows // LANES, step, start, unroll=2)
            for h in range(HIS):
                acc_pen[h, pl.ds(base, 8), :] = pens[h]
                acc_key[h, pl.ds(base, 8), :] = keys[h]

    best(0, 13)

    @pl.loop(1, PLANE)
    def _(k):
        plane_copy(k).wait()

    layer_box[layer] = jnp.sum(plane_box[...], axis=0)

    @pl.loop(1, LAYERS)
    def _(k):
        layer_copy(k).start()

    best(13, 16)

    for h in range(HIS):
        pen = fold_rows(acc_pen[h].T, jnp.maximum)[:1]
        key = fold_rows(acc_key[h].T, jnp.maximum)[:1]
        empty = pen <= 0.5 * LOWEST_FILL
        best_rank = jnp.where(empty, -1, lax.shift_right_arithmetic(key, 30) + 2)
        lowest_face = jnp.where(empty, FACE_LIMIT, FACE_LIMIT - 1 - (key & (FACE_LIMIT - 1)))
        if h < 8:
            own_f[rep, 0, h : h + 1, :] = pen
            own_i[rep, 0, h : h + 1, :] = best_rank
            own_i[rep, 1, h : h + 1, :] = lowest_face
        else:
            spill_f[0, h - 8 : h - 7, :] = pen
            spill_i[0, h - 8 : h - 7, :] = best_rank
            spill_i[1, h - 8 : h - 7, :] = lowest_face
    own_f[rep, 1] = seg_gap[:8]
    spill_f[1] = seg_gap[8:10]

    def own_copies(k):
        target = (dom, (rep + k) % REPS)
        return [
            pltpu.make_async_remote_copy(
                src_ref=box.at[rep], dst_ref=box.at[rep],
                send_sem=own_sem.at[0, j, k], recv_sem=own_sem.at[1, j, k],
                device_id=target, device_id_type=MESH,
            )
            for j, box in enumerate((own_f, own_i))
        ]

    def spill_copies(k):
        target = ((dom + 1) % DOMS, (rep + k) % REPS)
        return [
            pltpu.make_async_remote_copy(
                src_ref=source, dst_ref=box.at[rep],
                send_sem=spill_sem.at[0, j, k], recv_sem=spill_sem.at[1, j, k],
                device_id=target, device_id_type=MESH,
            )
            for j, (source, box) in enumerate(((spill_f, got_f), (spill_i, got_i)))
        ]

    sent = [copy for k in (2, 1, 3) for copy in own_copies(k)]
    sent += [copy for k in (2, 1, 3, 0) for copy in spill_copies(k)]
    for copy in sent:
        copy.start()

    ns = ns_buf[...]
    saved = []
    for c in range(chunks):
        part = pl.ds(c * CHUNK, CHUNK)
        force_buf[:, part] = jnp.dot(ns, loads[:, part], preferred_element_type=F32).astype(BF16)
        saved.append(pltpu.make_async_copy(force_buf.at[:, part], force_hbm.at[:, part], out_sem.at[c]))
        saved[-1].start()

    for copy in sent:
        copy.wait()

    def part_of(box_f, box_i, k):
        return box_f[k, 0], box_i[k, 0], box_i[k, 1], box_f[k, 1]

    total = part_of(own_f, own_i, 0)
    for k in range(1, REPS):
        total = combine(total, part_of(own_f, own_i, k))
    reach = part_of(got_f, got_i, 0)
    for k in range(1, REPS):
        reach = combine(reach, part_of(got_f, got_i, k))
    leading = combine([x[:2] for x in total], reach)
    for at, (pen, best_rank, face, gap_sum) in ((slice(0, 2), leading), (slice(2, 8), [x[2:] for x in total])):
        empty = best_rank < 0
        pen_out[at, :] = jnp.where(empty, 0.0, pen)
        face_out[at, :] = jnp.where(empty, -1, face)
        gap_out[at, :] = gap_sum

    @pl.loop(1, LAYERS)
    def _(k):
        layer_copy(k).wait()

    totals = jnp.sum(layer_box[...], axis=0)
    mean_out[...] = jnp.broadcast_to(totals[:, :1] / totals[:, 1:2], (1, LANES))
    for copy in saved:
        copy.wait()


def shards(ns, nm, sec, mst, off, qw, jac, slot, face, rank, live):
    rows = sec.shape[1]
    chunks = rows // CHUNK
    vmem = pl.BlockSpec(memory_space=pltpu.VMEM)
    hbm = pl.BlockSpec(memory_space=pl.ANY)
    smem = pl.BlockSpec(memory_space=pltpu.SMEM)

    def line(x):
        return x.reshape(1, -1)

    blocks = rows // LANES
    force, pen, face, gap, mean = pl.pallas_call(
        kernel,
        out_shape=(
            jax.ShapeDtypeStruct((K, rows), BF16),
            jax.ShapeDtypeStruct((8, LANES), F32),
            jax.ShapeDtypeStruct((8, LANES), I32),
            jax.ShapeDtypeStruct((8, LANES), F32),
            jax.ShapeDtypeStruct((1, LANES), F32),
        ),
        in_specs=[hbm] * 10 + [smem],
        out_specs=(hbm, vmem, vmem, vmem, vmem),
        scratch_shapes=[
            pltpu.VMEM((K, P_SIZE), BF16),
            pltpu.VMEM((K, P_SIZE), BF16),
            pltpu.VMEM((K, rows), BF16),
            pltpu.VMEM((K, rows), BF16),
            pltpu.VMEM((1, rows), F32),
            pltpu.VMEM((1, P_SIZE), F32),
            pltpu.VMEM((1, rows), F32),
            pltpu.VMEM((1, rows), I32),
            pltpu.VMEM((1, rows), I32),
            pltpu.VMEM((1, rows), I32),
            pltpu.VMEM((K, rows), BF16),
            pltpu.VMEM((P_SIZE, rows), BF16),
            pltpu.VMEM((P_SIZE + 16, 2 * LANES), BF16),
            pltpu.VMEM((P_SIZE, LANES), F32),
            pltpu.VMEM((blocks, 16, LANES), F32),
            pltpu.VMEM((blocks, 16, LANES), I32),
            pltpu.VMEM((blocks, 8, LANES), I32),
            pltpu.VMEM((HIS, LANES, LANES), F32),
            pltpu.VMEM((HIS, LANES, LANES), I32),
            pltpu.VMEM((PLANE, 1, LANES), F32),
            pltpu.VMEM((LAYERS, 1, LANES), F32),
            pltpu.VMEM((REPS, 2, 8, LANES), F32),
            pltpu.VMEM((REPS, 2, 8, LANES), I32),
            pltpu.VMEM((2, 2, LANES), F32),
            pltpu.VMEM((2, 2, LANES), I32),
            pltpu.VMEM((REPS, 2, 2, LANES), F32),
            pltpu.VMEM((REPS, 2, 2, LANES), I32),
            pltpu.SemaphoreType.DMA((2 * chunks + 8,)),
            pltpu.SemaphoreType.DMA((chunks,)),
            pltpu.SemaphoreType.DMA((2, PLANE)),
            pltpu.SemaphoreType.DMA((2, LAYERS)),
            pltpu.SemaphoreType.DMA((2, 2, REPS)),
            pltpu.SemaphoreType.DMA((2, 2, REPS)),
        ],
        compiler_params=pltpu.CompilerParams(
            vmem_limit_bytes=67_000_000, collective_id=0, has_side_effects=True
        ),
    )(ns, nm, sec, mst, line(off), line(qw), line(jac), line(slot), line(face), line(rank), live)
    return force, pen.reshape(-1), face.reshape(-1), gap.reshape(-1), mean[0, 0]


def solution(mesh):
    both = P(("dom", "rep"))
    return jax.shard_map(
        shards,
        mesh=mesh,
        in_specs=(P(), P(), P(None, ("dom", "rep")), P(None, ("dom", "rep")), both, P()) + (both,) * 5,
        out_specs=(P(None, ("dom", "rep")), P("dom"), P("dom"), P("dom"), P()),
        check_vma=False,
    )
```

```python
import jax
import jax.numpy as jnp
from jax import lax
from jax.experimental import pallas as pl
from jax.experimental.pallas import tpu as pltpu
from jax.sharding import PartitionSpec as P

P_SIZE = 256
K = 64
LANES = 128
HIS = 10
PENALTY = 400.0
LOWEST_FILL = -1e30
FACE_LIMIT = 1073741824
FACE_FILL = 3e38
LOW_BITS = 1 << 23
CHUNK = 1024
F32 = jnp.float32
I32 = jnp.int32
BF16 = jnp.bfloat16
MESH = pl.DeviceIdType.MESH
DOMS = 64
REPS = 4
PLANE_DOMS = 8
PLANE = PLANE_DOMS * REPS
LAYERS = DOMS // PLANE_DOMS
GREETED = PLANE - 1 + LAYERS - 1 + REPS


def pieces(x):
    high = x.astype(BF16)
    rest = x - high.astype(F32)
    mid = rest.astype(BF16)
    low = (rest - mid.astype(F32)).astype(BF16)
    return high.astype(F32), mid.astype(F32), low.astype(F32)


def fold_rows(x, op):
    while x.shape[0] > 8:
        half = x.shape[0] // 2
        x = op(x[:half], x[half:])
    for shift in (4, 2, 1):
        x = op(x, pltpu.roll(x, shift, 0))
    return x


def encoded(face):
    scale = jnp.full(face.shape, 2.0**-87, F32)
    for t in range(7):
        scale = jnp.where((face & (LOW_BITS << t)) != 0, scale * 2.0 ** (1 << t), scale)
    return ((face & (LOW_BITS - 1)) + LOW_BITS).astype(F32) * scale


def decoded(value):
    top = jnp.zeros(value.shape, I32)
    for t in range(6, -1, -1):
        above = value >= 2.0 ** ((1 << t) - 64)
        value = jnp.where(above, value * 2.0 ** -(1 << t), value)
        top = jnp.where(above, top + (LOW_BITS << t), top)
    return (value * 2.0**87).astype(I32) - LOW_BITS + top


def combine(earlier, latter):
    prefer = (latter[1] > earlier[1]) | (latter[1] == earlier[1]) & (latter[2] < earlier[2])
    return (
        jnp.maximum(earlier[0], latter[0]),
        jnp.where(prefer, latter[1], earlier[1]),
        jnp.where(prefer, latter[2], earlier[2]),
        earlier[3] + latter[3],
    )


def kernel(
    ns_hbm, nm_hbm, sec_hbm, mst_hbm, off_hbm, qw_hbm, jac_hbm, slot_hbm, face_hbm, rank_hbm, live_hbm,
    force_out, pen_out, face_out, gap_out, mean_out,
    ns_buf, nm_buf, sec_buf, mst_buf, off_buf, qw_buf, jac_buf, slot_buf, face_buf, rank_buf, live_buf,
    loads, table, weight, live_jac, hi_of, lo_of, mark, rank_f, face_f, one_hot, pen_by, face_by, acc,
    plane_box, layer_box, own_f, own_i, spill_f, spill_i, got_f, got_i,
    in_sem, plane_sem, layer_sem, own_sem, spill_sem,
):
    rows = sec_hbm.shape[1]
    chunks = rows // CHUNK
    per = CHUNK // LANES
    dom, rep = lax.axis_index("dom"), lax.axis_index("rep")
    layer, spot = dom // PLANE_DOMS, (dom % PLANE_DOMS) * REPS + rep

    def plane_device(k):
        other = (spot + k) % PLANE
        return layer * PLANE_DOMS + other // REPS, other % REPS

    def layer_device(k):
        return (layer + k) % LAYERS * PLANE_DOMS + dom % PLANE_DOMS, rep

    barrier = pltpu.get_barrier_semaphore()

    def greet(device):
        pl.semaphore_signal(barrier, inc=1, device_id=device, device_id_type=MESH)

    def load(c):
        part = pl.ds(c * CHUNK, CHUNK)
        return (
            pltpu.make_async_copy(sec_hbm.at[:, part], sec_buf.at[:, part], in_sem.at[c]),
            pltpu.make_async_copy(mst_hbm.at[:, part], mst_buf.at[:, part], in_sem.at[chunks + c]),
        )

    whole = (
        (ns_hbm, ns_buf), (nm_hbm, nm_buf), (qw_hbm, qw_buf), (live_hbm, live_buf), (jac_hbm, jac_buf),
        (slot_hbm, slot_buf), (face_hbm, face_buf), (rank_hbm, rank_buf), (off_hbm, off_buf),
    )
    singles = [pltpu.make_async_copy(a, b, in_sem.at[2 * chunks + k]) for k, (a, b) in enumerate(whole)]
    for copy in singles:
        copy.start()
    for c in range(chunks):
        for copy in load(c):
            copy.start()

    @pl.loop(1, PLANE)
    def _(k):
        greet(plane_device(k))

    @pl.loop(1, LAYERS)
    def _(k):
        greet(layer_device(k))

    @pl.loop(0, REPS)
    def _(k):
        greet(((dom + DOMS - 1) % DOMS, k))

    for copy in singles[:3]:
        copy.wait()
    ns = ns_buf[...]
    both = jnp.concatenate([ns.astype(F32), -nm_buf[...].astype(F32)], axis=0).T
    column = jnp.broadcast_to(qw_buf[...], (LANES, P_SIZE)).T
    weight[...] = column * (-PENALTY)
    total_weight = jnp.sum(qw_buf[...], axis=1, keepdims=True)
    coefficient = jnp.sum(both * column, axis=0, keepdims=True)
    high, mid, low = pieces(coefficient)
    eight = lax.broadcasted_iota(I32, (8, LANES), 0)
    extra = jnp.where(eight == 0, high, jnp.where(eight == 1, mid, jnp.where(eight == 2, low, 0.0)))
    table[...] = jnp.concatenate([both, extra, jnp.zeros_like(extra)], axis=0).astype(BF16)

    for copy in singles[3:]:
        copy.wait()
    blocks = rows // LANES
    row = lax.broadcasted_iota(I32, (blocks, LANES), 0) * LANES + lax.broadcasted_iota(I32, (blocks, LANES), 1)
    live = row < live_buf[...]
    slots, ranks = slot_buf[...], rank_buf[...]
    live_jac[...] = jnp.where(live, jac_buf[...], 0.0)
    hi_of[...] = jnp.where(live, lax.shift_right_logical(slots, 7), 99)
    lo_of[...] = slots & (LANES - 1)
    mark[...] = jnp.where(ranks == 3, 2.0**28, jnp.where(ranks == 2, 2.0**14, jnp.where(ranks == 1, 1.0, 0.0)))
    rank_f[...] = ranks.astype(F32)
    face_f[...] = encoded(face_buf[...])
    area = fold_rows(live_jac[...], jnp.add)[:1]
    area_total = jnp.sum(area, axis=1, keepdims=True) * total_weight

    whole_weight = jnp.broadcast_to(total_weight, (8, LANES))
    sixteen = lax.broadcasted_iota(I32, (16, LANES), 0)
    lo_ids = lax.broadcasted_iota(I32, (LANES, LANES), 0)
    sums = jnp.zeros((64, LANES), F32)
    for c in range(chunks):
        part = pl.ds(c * CHUNK, CHUNK)
        for copy in load(c):
            copy.wait()
        data = jnp.concatenate([sec_buf[:, part], mst_buf[:, part]], axis=0)
        found = jnp.dot(table[: P_SIZE + 8], data, preferred_element_type=F32)
        splits, marks = [], []
        for j in range(per):
            i = c * per + j
            at = slice(j * LANES, (j + 1) * LANES)
            offset = off_buf[pl.ds(i, 8, stride=0), :]
            gap = found[:P_SIZE, at].reshape(P_SIZE // 8, 8, LANES) + offset[None]
            row_pen = -fold_rows(jnp.min(gap, axis=0), jnp.minimum)
            push = jnp.maximum(weight[...].reshape(P_SIZE // 8, 8, LANES) * gap, 0.0)
            push = push * live_jac[pl.ds(i, 8, stride=0), :][None]
            loads[:, pl.ds(i * LANES, LANES)] = push.reshape(P_SIZE, LANES).astype(BF16)
            linear = fold_rows(found[P_SIZE : P_SIZE + 8, at], jnp.add)
            row_gap = jac_buf[pl.ds(i, 8, stride=0), :] * (linear + offset * whole_weight)
            member = hi_of[pl.ds(i, 16, stride=0), :] == sixteen
            pen_by[i] = jnp.where(member, jnp.concatenate([row_pen, row_pen], axis=0), LOWEST_FILL)
            terms = [jnp.concatenate([p, p], axis=0) for p in pieces(row_gap)]
            terms.append(mark[pl.ds(i, 16, stride=0), :])
            splits.append(jnp.concatenate([jnp.where(member, p, 0.0) for p in terms], axis=0).astype(BF16))
            lo = lo_of[pl.ds(i, 8, stride=0), :]
            same = lo_ids.reshape(LANES // 8, 8, LANES) == lo[None]
            marks.append(jnp.where(same, 1.0, 0.0).reshape(LANES, LANES).astype(BF16))
            one_hot[:, pl.ds(i * LANES, LANES)] = marks[-1]
        sums = sums + lax.dot_general(
            jnp.concatenate(splits, axis=1), jnp.concatenate(marks, axis=1), (((1,), (1,)), ((), ())),
            preferred_element_type=F32,
        )
    seg_gap = sums[:16] + sums[16:32] + sums[32:48]
    code = sums[48:]
    best_rank = jnp.where(code >= 2.0**28, 3.0, jnp.where(code >= 2.0**14, 2.0, jnp.where(code >= 1.0, 1.0, 0.0)))
    gap_total = jnp.sum(jnp.sum(seg_gap, axis=0, keepdims=True), axis=1, keepdims=True)
    first_lane = lax.broadcasted_iota(I32, (1, LANES), 1) == 0
    plane_box[spot] = jnp.where(first_lane, gap_total, area_total)

    def plane_copy(k):
        return pltpu.make_async_remote_copy(
            src_ref=plane_box.at[spot], dst_ref=plane_box.at[spot],
            send_sem=plane_sem.at[0, k], recv_sem=plane_sem.at[1, k],
            device_id=plane_device(k), device_id_type=MESH,
        )

    def layer_copy(k):
        return pltpu.make_async_remote_copy(
            src_ref=layer_box.at[layer], dst_ref=layer_box.at[layer],
            send_sem=layer_sem.at[0, k], recv_sem=layer_sem.at[1, k],
            device_id=layer_device(k), device_id_type=MESH,
        )

    def own_copy(j, box, k):
        return pltpu.make_async_remote_copy(
            src_ref=box.at[rep], dst_ref=box.at[rep],
            send_sem=own_sem.at[0, j, k], recv_sem=own_sem.at[1, j, k],
            device_id=(dom, (rep + k) % REPS), device_id_type=MESH,
        )

    def spill_copy(j, source, box, k):
        return pltpu.make_async_remote_copy(
            src_ref=source, dst_ref=box.at[rep],
            send_sem=spill_sem.at[0, j, k], recv_sem=spill_sem.at[1, j, k],
            device_id=((dom + 1) % DOMS, (rep + k) % REPS), device_id_type=MESH,
        )

    pl.semaphore_wait(barrier, GREETED)

    @pl.loop(1, PLANE)
    def _(k):
        plane_copy(k).start()

    group = 2

    def best(source, op, fill, first, last):
        @pl.loop(first, last)
        def _(g):
            base = pl.multiple_of(g * (8 * group), 8 * group)
            ids = [eight + (base + 8 * q) for q in range(group)]

            def step(i, carry):
                lo = lo_of[pl.ds(i, 8, stride=0), :]
                masks = [lo == ids[q] for q in range(group)]
                found = []
                for h in range(HIS):
                    value = source[i, pl.ds(h, 8, stride=0), :]
                    for q in range(group):
                        found.append(op(carry[h * group + q], jnp.where(masks[q], value, fill)))
                return found

            start = [jnp.full((8, LANES), fill, F32)] * (HIS * group)
            values = lax.fori_loop(0, blocks, step, start, unroll=4)
            for h in range(HIS):
                for q in range(group):
                    acc[h, pl.ds(base + 8 * q, 8), :] = values[h * group + q]

    turns = LANES // (8 * group)
    best(pen_by, jnp.maximum, LOWEST_FILL, 0, turns)

    for c in range(chunks):
        wanted = jnp.dot(
            best_rank.astype(BF16), one_hot[:, pl.ds(c * CHUNK, CHUNK)], preferred_element_type=F32
        )
        for j in range(per):
            i = c * per + j
            member = hi_of[pl.ds(i, 16, stride=0), :] == sixteen
            member = member & (wanted[:, j * LANES : (j + 1) * LANES] == rank_f[pl.ds(i, 16, stride=0), :])
            face_by[i] = jnp.where(member, face_f[pl.ds(i, 16, stride=0), :], FACE_FILL)

    seg_pen = [fold_rows(acc[h].T, jnp.maximum)[:1] for h in range(HIS)]
    lines = [(own_f.at[rep], h) for h in range(8)] + [(spill_f, h) for h in range(2)]
    for h, (box, at) in enumerate(lines):
        box[0, at : at + 1, :] = seg_pen[h]
        box[1, at : at + 1, :] = seg_gap[h : h + 1]
        box[2, at : at + 1, :] = jnp.where(seg_pen[h] <= 0.5 * LOWEST_FILL, -1.0, best_rank[h : h + 1])

    sent = [own_copy(0, own_f, k) for k in (2, 1, 3)]
    sent += [spill_copy(0, spill_f, got_f, k) for k in (2, 1, 3, 0)]
    for copy in sent:
        copy.start()

    best(face_by, jnp.minimum, FACE_FILL, 0, turns // 2)

    @pl.loop(1, PLANE)
    def _(k):
        plane_copy(k).wait()

    layer_box[layer] = jnp.sum(plane_box[...], axis=0)

    @pl.loop(1, LAYERS)
    def _(k):
        layer_copy(k).start()

    best(face_by, jnp.minimum, FACE_FILL, turns // 2, turns)

    for h in range(HIS):
        value = fold_rows(acc[h].T, jnp.minimum)[:1]
        face = jnp.where(seg_pen[h] <= 0.5 * LOWEST_FILL, FACE_LIMIT, decoded(value))
        if h < 8:
            own_i[rep, h : h + 1, :] = face
        else:
            spill_i[h - 8 : h - 7, :] = face

    later = [own_copy(1, own_i, k) for k in (2, 1, 3)]
    later += [spill_copy(1, spill_i, got_i, k) for k in (2, 1, 3, 0)]
    for copy in later:
        copy.start()

    ns = ns_buf[...]
    for c in range(chunks):
        part = pl.ds(c * CHUNK, CHUNK)
        force_out[:, part] = jnp.dot(ns, loads[:, part], preferred_element_type=F32).astype(BF16)

    for copy in sent + later:
        copy.wait()

    def part_of(box_f, box_i, k):
        return box_f[k, 0], box_f[k, 2], box_i[k], box_f[k, 1]

    total = part_of(own_f, own_i, 0)
    for k in range(1, REPS):
        total = combine(total, part_of(own_f, own_i, k))
    reach = part_of(got_f, got_i, 0)
    for k in range(1, REPS):
        reach = combine(reach, part_of(got_f, got_i, k))
    leading = combine([x[:2] for x in total], reach)
    for at, (pen, top, face, gap_sum) in ((slice(0, 2), leading), (slice(2, 8), [x[2:] for x in total])):
        empty = top < 0.0
        pen_out[at, :] = jnp.where(empty, 0.0, pen)
        face_out[at, :] = jnp.where(empty, -1, face)
        gap_out[at, :] = gap_sum

    @pl.loop(1, LAYERS)
    def _(k):
        layer_copy(k).wait()

    totals = jnp.sum(layer_box[...], axis=0)
    mean_out[...] = jnp.broadcast_to(totals[:, :1] / totals[:, 1:2], (1, LANES))


def write_out(*refs):
    count = (len(refs) - 1) // 2
    copies = [pltpu.make_async_copy(refs[k], refs[count + k], refs[-1].at[k]) for k in range(count)]
    for copy in copies:
        copy.start()
    for copy in copies:
        copy.wait()


def shards(ns, nm, sec, mst, off, qw, jac, slot, face, rank, live):
    rows = sec.shape[1]
    chunks, blocks = rows // CHUNK, rows // LANES
    vmem = pl.BlockSpec(memory_space=pltpu.VMEM)
    hbm = pl.BlockSpec(memory_space=pl.ANY)

    def dense(x):
        return x.reshape(blocks, LANES)

    shapes = [((K, rows), BF16), ((8, LANES), F32), ((8, LANES), I32), ((8, LANES), F32), ((1, LANES), F32)]
    results = pl.pallas_call(
        kernel,
        out_shape=[pltpu.VMEM(shape, kind) for shape, kind in shapes],
        in_specs=[hbm] * 11,
        out_specs=[vmem] * 5,
        scratch_shapes=[
            pltpu.VMEM((K, P_SIZE), BF16),
            pltpu.VMEM((K, P_SIZE), BF16),
            pltpu.VMEM((K, rows), BF16),
            pltpu.VMEM((K, rows), BF16),
            pltpu.VMEM((blocks, LANES), F32),
            pltpu.VMEM((1, P_SIZE), F32),
            pltpu.VMEM((blocks, LANES), F32),
            pltpu.VMEM((blocks, LANES), I32),
            pltpu.VMEM((blocks, LANES), I32),
            pltpu.VMEM((blocks, LANES), I32),
            pltpu.VMEM((1, 1), I32),
            pltpu.VMEM((P_SIZE, rows), BF16),
            pltpu.VMEM((P_SIZE + 16, LANES), BF16),
            pltpu.VMEM((P_SIZE, LANES), F32),
            pltpu.VMEM((blocks, LANES), F32),
            pltpu.VMEM((blocks, LANES), I32),
            pltpu.VMEM((blocks, LANES), I32),
            pltpu.VMEM((blocks, LANES), F32),
            pltpu.VMEM((blocks, LANES), F32),
            pltpu.VMEM((blocks, LANES), F32),
            pltpu.VMEM((LANES, rows), BF16),
            pltpu.VMEM((blocks, 16, LANES), F32),
            pltpu.VMEM((blocks, 16, LANES), F32),
            pltpu.VMEM((HIS, LANES, LANES), F32),
            pltpu.VMEM((PLANE, 1, LANES), F32),
            pltpu.VMEM((LAYERS, 1, LANES), F32),
            pltpu.VMEM((REPS, 3, 8, LANES), F32),
            pltpu.VMEM((REPS, 8, LANES), I32),
            pltpu.VMEM((3, 2, LANES), F32),
            pltpu.VMEM((2, LANES), I32),
            pltpu.VMEM((REPS, 3, 2, LANES), F32),
            pltpu.VMEM((REPS, 2, LANES), I32),
            pltpu.SemaphoreType.DMA((2 * chunks + 9,)),
            pltpu.SemaphoreType.DMA((2, PLANE)),
            pltpu.SemaphoreType.DMA((2, LAYERS)),
            pltpu.SemaphoreType.DMA((2, 2, REPS)),
            pltpu.SemaphoreType.DMA((2, 2, REPS)),
        ],
        compiler_params=pltpu.CompilerParams(
            vmem_limit_bytes=64_000_000, collective_id=0, has_side_effects=True
        ),
    )(ns, nm, sec, mst, dense(off), qw.reshape(1, -1), dense(jac), dense(slot), dense(face), dense(rank), live.reshape(1, 1))
    force, pen, face, gap, mean = pl.pallas_call(
        write_out,
        out_shape=[jax.ShapeDtypeStruct(shape, kind) for shape, kind in shapes],
        in_specs=[vmem] * 5,
        out_specs=[hbm] * 5,
        scratch_shapes=[pltpu.SemaphoreType.DMA((5,))],
        compiler_params=pltpu.CompilerParams(vmem_limit_bytes=1 << 20),
    )(*results)
    return force, pen.reshape(-1), face.reshape(-1), gap.reshape(-1), mean[0, 0]


def solution(mesh):
    both = P(("dom", "rep"))
    return jax.shard_map(
        shards,
        mesh=mesh,
        in_specs=(P(), P(), P(None, ("dom", "rep")), P(None, ("dom", "rep")), both, P()) + (both,) * 5,
        out_specs=(P(None, ("dom", "rep")), P("dom"), P("dom"), P("dom"), P()),
        check_vma=False,
    )
```

```python
import jax
import jax.numpy as jnp
from jax import lax
from jax.experimental import pallas as pl
from jax.experimental.pallas import tpu as pltpu
from jax.sharding import PartitionSpec as P

P_SIZE = 256
K = 64
LANES = 128
HIS = 10
PENALTY = 400.0
LOWEST_FILL = -1e30
FACE_LIMIT = 1073741824
FACE_FILL = 3e38
LOW_BITS = 1 << 23
CHUNK = 1024
F32 = jnp.float32
I32 = jnp.int32
BF16 = jnp.bfloat16
MESH = pl.DeviceIdType.MESH
DOMS = 64
REPS = 4
PLANE_DOMS = 8
PLANE = PLANE_DOMS * REPS
LAYERS = DOMS // PLANE_DOMS
GREETED = PLANE - 1 + LAYERS - 1 + REPS


def pieces(x):
    high = x.astype(BF16)
    rest = x - high.astype(F32)
    mid = rest.astype(BF16)
    low = (rest - mid.astype(F32)).astype(BF16)
    return high.astype(F32), mid.astype(F32), low.astype(F32)


def fold_rows(x, op):
    while x.shape[0] > 8:
        half = x.shape[0] // 2
        x = op(x[:half], x[half:])
    for shift in (4, 2, 1):
        x = op(x, pltpu.roll(x, shift, 0))
    return x


def encoded(face):
    scale = jnp.full(face.shape, 2.0**-87, F32)
    for t in range(7):
        scale = jnp.where((face & (LOW_BITS << t)) != 0, scale * 2.0 ** (1 << t), scale)
    return ((face & (LOW_BITS - 1)) + LOW_BITS).astype(F32) * scale


def decoded(value):
    top = jnp.zeros(value.shape, I32)
    for t in range(6, -1, -1):
        above = value >= 2.0 ** ((1 << t) - 64)
        value = jnp.where(above, value * 2.0 ** -(1 << t), value)
        top = jnp.where(above, top + (LOW_BITS << t), top)
    return (value * 2.0**87).astype(I32) - LOW_BITS + top


def combine(earlier, latter):
    prefer = (latter[1] > earlier[1]) | (latter[1] == earlier[1]) & (latter[2] < earlier[2])
    return (
        jnp.maximum(earlier[0], latter[0]),
        jnp.where(prefer, latter[1], earlier[1]),
        jnp.where(prefer, latter[2], earlier[2]),
        earlier[3] + latter[3],
    )


def kernel(
    ns_hbm, nm_hbm, sec_hbm, mst_hbm, off_hbm, qw_hbm, jac_hbm, slot_hbm, face_hbm, rank_hbm, live_hbm,
    force_out, pen_out, face_out, gap_out, mean_out,
    ns_buf, nm_buf, sec_buf, mst_buf, off_buf, qw_buf, jac_buf, slot_buf, face_buf, rank_buf, live_buf,
    table, weight, live_jac, hi_of, lo_of, lo_f, mark, rank_f, face_f, one_hot, pen_by, face_by, acc,
    plane_box, layer_box, own_f, own_i, spill_f, spill_i, got_f, got_i,
    in_sem, plane_sem, layer_sem, own_sem, spill_sem,
):
    rows = sec_hbm.shape[1]
    chunks = rows // CHUNK
    per = CHUNK // LANES
    dom, rep = lax.axis_index("dom"), lax.axis_index("rep")
    layer, spot = dom >> 3, (dom & 7) * REPS + rep

    def plane_device(k):
        other = (spot + k) & (PLANE - 1)
        return layer * PLANE_DOMS + (other >> 2), other & 3

    def layer_device(k):
        return ((layer + k) & (LAYERS - 1)) * PLANE_DOMS + (dom & 7), rep

    barrier = pltpu.get_barrier_semaphore()

    def greet(device):
        pl.semaphore_signal(barrier, inc=1, device_id=device, device_id_type=MESH)

    def load(c):
        part = pl.ds(c * CHUNK, CHUNK)
        return (
            pltpu.make_async_copy(sec_hbm.at[:, part], sec_buf.at[:, part], in_sem.at[c]),
            pltpu.make_async_copy(mst_hbm.at[:, part], mst_buf.at[:, part], in_sem.at[chunks + c]),
        )

    whole = (
        (ns_hbm, ns_buf), (nm_hbm, nm_buf), (qw_hbm, qw_buf), (live_hbm, live_buf), (jac_hbm, jac_buf),
        (slot_hbm, slot_buf), (face_hbm, face_buf), (rank_hbm, rank_buf), (off_hbm, off_buf),
    )
    singles = [pltpu.make_async_copy(a, b, in_sem.at[2 * chunks + k]) for k, (a, b) in enumerate(whole)]
    for copy in singles:
        copy.start()
    for c in range(chunks):
        for copy in load(c):
            copy.start()

    @pl.loop(1, PLANE)
    def _(k):
        greet(plane_device(k))

    @pl.loop(1, LAYERS)
    def _(k):
        greet(layer_device(k))

    @pl.loop(0, REPS)
    def _(k):
        greet(((dom + DOMS - 1) & (DOMS - 1), k))

    for copy in singles[:3]:
        copy.wait()
    ns = ns_buf[...]
    both = jnp.concatenate([ns.astype(F32), -nm_buf[...].astype(F32)], axis=0).T
    column = jnp.broadcast_to(qw_buf[...], (LANES, P_SIZE)).T
    weight[...] = column * (-PENALTY)
    total_weight = jnp.sum(qw_buf[...], axis=1, keepdims=True)
    coefficient = jnp.sum(both * column, axis=0, keepdims=True)
    high, mid, low = pieces(coefficient)
    eight = lax.broadcasted_iota(I32, (8, LANES), 0)
    extra = jnp.where(eight == 0, high, jnp.where(eight == 1, mid, jnp.where(eight == 2, low, 0.0)))
    table[...] = jnp.concatenate([both, extra, jnp.zeros_like(extra)], axis=0).astype(BF16)

    for copy in singles[3:]:
        copy.wait()
    blocks = rows // LANES
    row = lax.broadcasted_iota(I32, (blocks, LANES), 0) * LANES + lax.broadcasted_iota(I32, (blocks, LANES), 1)
    live = row < live_buf[...]
    slots, ranks = slot_buf[...], rank_buf[...]
    live_jac[...] = jnp.where(live, jac_buf[...], 0.0)
    hi_of[...] = jnp.where(live, lax.shift_right_logical(slots, 7), 99)
    lo_of[...] = slots & (LANES - 1)
    lo_f[...] = (slots & (LANES - 1)).astype(F32)
    mark[...] = jnp.where(ranks == 3, 2.0**28, jnp.where(ranks == 2, 2.0**14, jnp.where(ranks == 1, 1.0, 0.0)))
    rank_f[...] = ranks.astype(F32)
    face_f[...] = encoded(face_buf[...])
    area = fold_rows(live_jac[...], jnp.add)[:1]
    area_total = jnp.sum(area, axis=1, keepdims=True) * total_weight

    whole_weight = jnp.broadcast_to(total_weight, (8, LANES))
    sixteen = lax.broadcasted_iota(I32, (16, LANES), 0)
    lo_ids = lax.broadcasted_iota(I32, (LANES, LANES), 0).astype(F32).astype(BF16)
    sums = jnp.zeros((64, LANES), F32)
    for c in range(chunks):
        for copy in load(c):
            copy.wait()

    def project(c, width, count):
        part = pl.ds(c * width, width)
        data = jnp.concatenate([sec_buf[:, part], mst_buf[:, part]], axis=0)
        return jnp.dot(table[:count], data, preferred_element_type=F32)

    ahead = project(0, CHUNK, P_SIZE + 8)
    for c in range(chunks):
        found = ahead
        if c + 1 < chunks:
            ahead = project(c + 1, CHUNK, P_SIZE + 8)
        splits, marks = [], []
        for j in range(per):
            i = c * per + j
            at = slice(j * LANES, (j + 1) * LANES)
            offset = off_buf[pl.ds(i, 8, stride=0), :]
            row_pen = -(fold_rows(found[:P_SIZE, at], jnp.minimum) + offset)
            linear = fold_rows(found[P_SIZE : P_SIZE + 8, at], jnp.add)
            row_gap = jac_buf[pl.ds(i, 8, stride=0), :] * (linear + offset * whole_weight)
            member = hi_of[pl.ds(i, 16, stride=0), :] == sixteen
            pen_by[i] = jnp.where(member, jnp.concatenate([row_pen, row_pen], axis=0), LOWEST_FILL)
            terms = [jnp.concatenate([p, p], axis=0) for p in pieces(row_gap)]
            terms.append(mark[pl.ds(i, 16, stride=0), :])
            splits.append(jnp.concatenate([jnp.where(member, p, 0.0) for p in terms], axis=0).astype(BF16))
            lo = lo_f[pl.ds(i, 16, stride=0), :].astype(BF16)
            same = lo_ids.reshape(LANES // 16, 16, LANES) == lo[None]
            marks.append(jnp.where(same, jnp.bfloat16(1), jnp.bfloat16(0)).reshape(LANES, LANES))
            one_hot[:, pl.ds(i * LANES, LANES)] = marks[-1]
        sums = sums + lax.dot_general(
            jnp.concatenate(splits, axis=1), jnp.concatenate(marks, axis=1), (((1,), (1,)), ((), ())),
            preferred_element_type=F32,
        )
    seg_gap = sums[:16] + sums[16:32] + sums[32:48]
    code = sums[48:]
    best_rank = jnp.where(code >= 2.0**28, 3.0, jnp.where(code >= 2.0**14, 2.0, jnp.where(code >= 1.0, 1.0, 0.0)))
    gap_total = jnp.sum(jnp.sum(seg_gap, axis=0, keepdims=True), axis=1, keepdims=True)
    first_lane = lax.broadcasted_iota(I32, (1, LANES), 1) == 0
    plane_box[spot] = jnp.where(first_lane, gap_total, area_total)

    def plane_copy(k):
        return pltpu.make_async_remote_copy(
            src_ref=plane_box.at[spot], dst_ref=plane_box.at[spot],
            send_sem=plane_sem.at[0, k], recv_sem=plane_sem.at[1, k],
            device_id=plane_device(k), device_id_type=MESH,
        )

    def layer_copy(k):
        return pltpu.make_async_remote_copy(
            src_ref=layer_box.at[layer], dst_ref=layer_box.at[layer],
            send_sem=layer_sem.at[0, k], recv_sem=layer_sem.at[1, k],
            device_id=layer_device(k), device_id_type=MESH,
        )

    def own_copy(j, box, k):
        return pltpu.make_async_remote_copy(
            src_ref=box.at[rep], dst_ref=box.at[rep],
            send_sem=own_sem.at[0, j, k], recv_sem=own_sem.at[1, j, k],
            device_id=(dom, (rep + k) & (REPS - 1)), device_id_type=MESH,
        )

    def spill_copy(j, source, box, k):
        return pltpu.make_async_remote_copy(
            src_ref=source, dst_ref=box.at[rep],
            send_sem=spill_sem.at[0, j, k], recv_sem=spill_sem.at[1, j, k],
            device_id=((dom + 1) & (DOMS - 1), (rep + k) & (REPS - 1)), device_id_type=MESH,
        )

    pl.semaphore_wait(barrier, GREETED)

    @pl.loop(1, PLANE)
    def _(k):
        plane_copy(k).start()

    group = 2

    def best(source, op, fill, first, last):
        @pl.loop(first, last)
        def _(g):
            base = pl.multiple_of(g * (8 * group), 8 * group)
            ids = [eight + (base + 8 * q) for q in range(group)]

            def step(i, carry):
                lo = lo_of[pl.ds(i, 8, stride=0), :]
                masks = [lo == ids[q] for q in range(group)]
                found = []
                for h in range(HIS):
                    value = source[i, pl.ds(h, 8, stride=0), :]
                    for q in range(group):
                        found.append(op(carry[h * group + q], jnp.where(masks[q], value, fill)))
                return found

            start = [jnp.full((8, LANES), fill, F32)] * (HIS * group)
            values = lax.fori_loop(0, blocks, step, start, unroll=8)
            for h in range(HIS):
                for q in range(group):
                    acc[h, pl.ds(base + 8 * q, 8), :] = values[h * group + q]

    turns = LANES // (8 * group)
    best(pen_by, jnp.maximum, LOWEST_FILL, 0, turns)

    for c in range(chunks):
        wanted = jnp.dot(
            best_rank.astype(BF16), one_hot[:, pl.ds(c * CHUNK, CHUNK)], preferred_element_type=F32
        )
        for j in range(per):
            i = c * per + j
            member = hi_of[pl.ds(i, 16, stride=0), :] == sixteen
            member = member & (wanted[:, j * LANES : (j + 1) * LANES] == rank_f[pl.ds(i, 16, stride=0), :])
            face_by[i] = jnp.where(member, face_f[pl.ds(i, 16, stride=0), :], FACE_FILL)

    seg_pen = [fold_rows(acc[h].T, jnp.maximum)[:1] for h in range(HIS)]
    lines = [(own_f.at[rep], h) for h in range(8)] + [(spill_f, h) for h in range(2)]
    for h, (box, at) in enumerate(lines):
        box[0, at : at + 1, :] = seg_pen[h]
        box[1, at : at + 1, :] = seg_gap[h : h + 1]
        box[2, at : at + 1, :] = jnp.where(seg_pen[h] <= 0.5 * LOWEST_FILL, -1.0, best_rank[h : h + 1])

    sent = [own_copy(0, own_f, k) for k in (2, 1, 3)]
    sent += [spill_copy(0, spill_f, got_f, k) for k in (2, 1, 3, 0)]
    for copy in sent:
        copy.start()

    best(face_by, jnp.minimum, FACE_FILL, 0, turns // 2)

    @pl.loop(1, PLANE)
    def _(k):
        plane_copy(k).wait()

    layer_box[layer] = jnp.sum(plane_box[...], axis=0)

    @pl.loop(1, LAYERS)
    def _(k):
        layer_copy(k).start()

    best(face_by, jnp.minimum, FACE_FILL, turns // 2, turns)

    for h in range(HIS):
        value = fold_rows(acc[h].T, jnp.minimum)[:1]
        face = jnp.where(seg_pen[h] <= 0.5 * LOWEST_FILL, FACE_LIMIT, decoded(value))
        if h < 8:
            own_i[rep, h : h + 1, :] = face
        else:
            spill_i[h - 8 : h - 7, :] = face

    later = [own_copy(1, own_i, k) for k in (2, 1, 3)]
    later += [spill_copy(1, spill_i, got_i, k) for k in (2, 1, 3, 0)]
    for copy in later:
        copy.start()

    ns = ns_buf[...]
    half = 256
    ns = ns_buf[...]
    turns_of = rows // half

    def push_of(c, found):
        pushes = []
        for j in range(half // LANES):
            i = c * (half // LANES) + j
            gap = found[:, j * LANES : (j + 1) * LANES].reshape(P_SIZE // 8, 8, LANES)
            gap = gap + off_buf[pl.ds(i, 8, stride=0), :][None]
            push = jnp.maximum(weight[...].reshape(P_SIZE // 8, 8, LANES) * gap, 0.0)
            push = push * live_jac[pl.ds(i, 8, stride=0), :][None]
            pushes.append(push.reshape(P_SIZE, LANES).astype(BF16))
        return jnp.concatenate(pushes, axis=1)

    ahead, ready = project(0, half, P_SIZE), None
    for c in range(turns_of + 1):
        now = ahead
        if c + 1 < turns_of:
            ahead = project(c + 1, half, P_SIZE)
        if ready is not None:
            force_out[:, pl.ds((c - 1) * half, half)] = jnp.dot(ns, ready, preferred_element_type=F32).astype(BF16)
        if c < turns_of:
            ready = push_of(c, now)

    for copy in sent + later:
        copy.wait()

    def part_of(box_f, box_i, k):
        return box_f[k, 0], box_f[k, 2], box_i[k], box_f[k, 1]

    total = part_of(own_f, own_i, 0)
    for k in range(1, REPS):
        total = combine(total, part_of(own_f, own_i, k))
    reach = part_of(got_f, got_i, 0)
    for k in range(1, REPS):
        reach = combine(reach, part_of(got_f, got_i, k))
    leading = combine([x[:2] for x in total], reach)
    for at, (pen, top, face, gap_sum) in ((slice(0, 2), leading), (slice(2, 8), [x[2:] for x in total])):
        empty = top < 0.0
        pen_out[at, :] = jnp.where(empty, 0.0, pen)
        face_out[at, :] = jnp.where(empty, -1, face)
        gap_out[at, :] = gap_sum

    @pl.loop(1, LAYERS)
    def _(k):
        layer_copy(k).wait()

    totals = jnp.sum(layer_box[...], axis=0)
    mean_out[...] = jnp.broadcast_to(totals[:, :1] / totals[:, 1:2], (1, LANES))


def write_out(*refs):
    count = (len(refs) - 1) // 2
    copies = [pltpu.make_async_copy(refs[k], refs[count + k], refs[-1].at[k]) for k in range(count)]
    for copy in copies:
        copy.start()
    for copy in copies:
        copy.wait()


def shards(ns, nm, sec, mst, off, qw, jac, slot, face, rank, live):
    rows = sec.shape[1]
    chunks, blocks = rows // CHUNK, rows // LANES
    vmem = pl.BlockSpec(memory_space=pltpu.VMEM)
    hbm = pl.BlockSpec(memory_space=pl.ANY)

    def dense(x):
        return x.reshape(blocks, LANES)

    shapes = [((K, rows), BF16), ((8, LANES), F32), ((8, LANES), I32), ((8, LANES), F32), ((1, LANES), F32)]
    results = pl.pallas_call(
        kernel,
        out_shape=[pltpu.VMEM(shape, kind) for shape, kind in shapes],
        in_specs=[hbm] * 11,
        out_specs=[vmem] * 5,
        scratch_shapes=[
            pltpu.VMEM((K, P_SIZE), BF16),
            pltpu.VMEM((K, P_SIZE), BF16),
            pltpu.VMEM((K, rows), BF16),
            pltpu.VMEM((K, rows), BF16),
            pltpu.VMEM((blocks, LANES), F32),
            pltpu.VMEM((1, P_SIZE), F32),
            pltpu.VMEM((blocks, LANES), F32),
            pltpu.VMEM((blocks, LANES), I32),
            pltpu.VMEM((blocks, LANES), I32),
            pltpu.VMEM((blocks, LANES), I32),
            pltpu.VMEM((1, 1), I32),
            pltpu.VMEM((P_SIZE + 16, LANES), BF16),
            pltpu.VMEM((P_SIZE, LANES), F32),
            pltpu.VMEM((blocks, LANES), F32),
            pltpu.VMEM((blocks, LANES), I32),
            pltpu.VMEM((blocks, LANES), I32),
            pltpu.VMEM((blocks, LANES), F32),
            pltpu.VMEM((blocks, LANES), F32),
            pltpu.VMEM((blocks, LANES), F32),
            pltpu.VMEM((blocks, LANES), F32),
            pltpu.VMEM((LANES, rows), BF16),
            pltpu.VMEM((blocks, 16, LANES), F32),
            pltpu.VMEM((blocks, 16, LANES), F32),
            pltpu.VMEM((HIS, LANES, LANES), F32),
            pltpu.VMEM((PLANE, 1, LANES), F32),
            pltpu.VMEM((LAYERS, 1, LANES), F32),
            pltpu.VMEM((REPS, 3, 8, LANES), F32),
            pltpu.VMEM((REPS, 8, LANES), I32),
            pltpu.VMEM((3, 2, LANES), F32),
            pltpu.VMEM((2, LANES), I32),
            pltpu.VMEM((REPS, 3, 2, LANES), F32),
            pltpu.VMEM((REPS, 2, LANES), I32),
            pltpu.SemaphoreType.DMA((2 * chunks + 9,)),
            pltpu.SemaphoreType.DMA((2, PLANE)),
            pltpu.SemaphoreType.DMA((2, LAYERS)),
            pltpu.SemaphoreType.DMA((2, 2, REPS)),
            pltpu.SemaphoreType.DMA((2, 2, REPS)),
        ],
        compiler_params=pltpu.CompilerParams(
            vmem_limit_bytes=64_000_000, collective_id=0, has_side_effects=True
        ),
    )(ns, nm, sec, mst, dense(off), qw.reshape(1, -1), dense(jac), dense(slot), dense(face), dense(rank), live.reshape(1, 1))
    force, pen, face, gap, mean = pl.pallas_call(
        write_out,
        out_shape=[jax.ShapeDtypeStruct(shape, kind) for shape, kind in shapes],
        in_specs=[vmem] * 5,
        out_specs=[hbm] * 5,
        scratch_shapes=[pltpu.SemaphoreType.DMA((5,))],
        compiler_params=pltpu.CompilerParams(vmem_limit_bytes=1 << 20),
    )(*results)
    return force, pen.reshape(-1), face.reshape(-1), gap.reshape(-1), mean[0, 0]


def solution(mesh):
    both = P(("dom", "rep"))
    return jax.shard_map(
        shards,
        mesh=mesh,
        in_specs=(P(), P(), P(None, ("dom", "rep")), P(None, ("dom", "rep")), both, P()) + (both,) * 5,
        out_specs=(P(None, ("dom", "rep")), P("dom"), P("dom"), P("dom"), P()),
        check_vma=False,
    )
```

```python
import jax
import jax.numpy as jnp
from jax import lax
from jax.experimental import pallas as pl
from jax.experimental.pallas import tpu as pltpu
from jax.sharding import PartitionSpec as P

P_SIZE = 256
K = 64
LANES = 128
HIS = 10
PENALTY = 400.0
LOWEST_FILL = -1e30
FACE_LIMIT = 1073741824
FACE_FILL = 3e38
LOW_BITS = 1 << 23
CHUNK = 1024
PARTS = 2
F32 = jnp.float32
I32 = jnp.int32
BF16 = jnp.bfloat16
MESH = pl.DeviceIdType.MESH
DOMS = 64
REPS = 4
PLANE_DOMS = 8
PLANE = PLANE_DOMS * REPS
LAYERS = DOMS // PLANE_DOMS
GREETED = PLANE - 1 + LAYERS - 1 + REPS


def pieces(x):
    high = x.astype(BF16)
    rest = x - high.astype(F32)
    mid = rest.astype(BF16)
    low = (rest - mid.astype(F32)).astype(BF16)
    return high.astype(F32), mid.astype(F32), low.astype(F32)


def fold_rows(x, op):
    while x.shape[0] > 8:
        half = x.shape[0] // 2
        x = op(x[:half], x[half:])
    for shift in (4, 2, 1):
        x = op(x, pltpu.roll(x, shift, 0))
    return x


def encoded(face):
    scale = jnp.full(face.shape, 2.0**-87, F32)
    for t in range(7):
        scale = jnp.where((face & (LOW_BITS << t)) != 0, scale * 2.0 ** (1 << t), scale)
    return ((face & (LOW_BITS - 1)) + LOW_BITS).astype(F32) * scale


def decoded(value):
    top = jnp.zeros(value.shape, I32)
    for t in range(6, -1, -1):
        above = value >= 2.0 ** ((1 << t) - 64)
        value = jnp.where(above, value * 2.0 ** -(1 << t), value)
        top = jnp.where(above, top + (LOW_BITS << t), top)
    return (value * 2.0**87).astype(I32) - LOW_BITS + top


def combine(earlier, latter):
    prefer = (latter[1] > earlier[1]) | (latter[1] == earlier[1]) & (latter[2] < earlier[2])
    return (
        jnp.maximum(earlier[0], latter[0]),
        jnp.where(prefer, latter[1], earlier[1]),
        jnp.where(prefer, latter[2], earlier[2]),
        earlier[3] + latter[3],
    )


def kernel(
    ns_hbm, nm_hbm, sec_hbm, mst_hbm, off_hbm, qw_hbm, jac_hbm, slot_hbm, face_hbm, rank_hbm, live_hbm,
    force_out, pen_out, face_out, gap_out, mean_out,
    ns_buf, nm_buf, sec_buf, mst_buf, off_buf, qw_buf, jac_buf, slot_buf, face_buf, rank_buf, live_buf,
    table, weight, live_jac, hi_of, lo_of, lo_f, mark, rank_f, face_f, one_hot, pen_by, face_by, acc_pen, acc_face,
    plane_box, layer_box, own_f, own_i, spill_f, spill_i, got_f, got_i,
    in_sem, plane_sem, layer_sem, own_sem, spill_sem,
):
    rows = sec_hbm.shape[1]
    chunks = rows // CHUNK
    per = CHUNK // LANES
    dom, rep = lax.axis_index("dom"), lax.axis_index("rep")
    layer, spot = dom >> 3, (dom & 7) * REPS + rep

    def plane_device(k):
        other = (spot + k) & (PLANE - 1)
        return layer * PLANE_DOMS + (other >> 2), other & 3

    def layer_device(k):
        return ((layer + k) & (LAYERS - 1)) * PLANE_DOMS + (dom & 7), rep

    barrier = pltpu.get_barrier_semaphore()

    def greet(device):
        pl.semaphore_signal(barrier, inc=1, device_id=device, device_id_type=MESH)

    def load(c):
        part = pl.ds(c * (rows // PARTS), rows // PARTS)
        return (
            pltpu.make_async_copy(sec_hbm.at[:, part], sec_buf.at[:, part], in_sem.at[c]),
            pltpu.make_async_copy(mst_hbm.at[:, part], mst_buf.at[:, part], in_sem.at[PARTS + c]),
        )

    whole = (
        (ns_hbm, ns_buf), (nm_hbm, nm_buf), (qw_hbm, qw_buf), (live_hbm, live_buf), (jac_hbm, jac_buf),
        (slot_hbm, slot_buf), (face_hbm, face_buf), (rank_hbm, rank_buf), (off_hbm, off_buf),
    )
    singles = [pltpu.make_async_copy(a, b, in_sem.at[2 * PARTS + k]) for k, (a, b) in enumerate(whole)]
    @pl.loop(1, LAYERS)
    def _(k):
        greet(layer_device(k))

    for copy in singles:
        copy.start()
    for c in range(PARTS):
        for copy in load(c):
            copy.start()

    @pl.loop(1, PLANE)
    def _(k):
        greet(plane_device(k))

    @pl.loop(0, REPS)
    def _(k):
        greet(((dom + DOMS - 1) & (DOMS - 1), k))

    for copy in singles[:3]:
        copy.wait()
    ns = ns_buf[...]
    both = jnp.concatenate([ns.astype(F32), -nm_buf[...].astype(F32)], axis=0).T
    column = jnp.broadcast_to(qw_buf[...], (LANES, P_SIZE)).T
    weight[...] = column * (-PENALTY)
    total_weight = jnp.sum(qw_buf[...], axis=1, keepdims=True)
    coefficient = jnp.sum(both * column, axis=0, keepdims=True)
    high, mid, low = pieces(coefficient)
    eight = lax.broadcasted_iota(I32, (8, LANES), 0)
    extra = jnp.where(eight == 0, high, jnp.where(eight == 1, mid, jnp.where(eight == 2, low, 0.0)))
    table[...] = jnp.concatenate([both, extra, jnp.zeros_like(extra)], axis=0).astype(BF16)

    for copy in singles[3:]:
        copy.wait()
    blocks = rows // LANES
    row = lax.broadcasted_iota(I32, (blocks, LANES), 0) * LANES + lax.broadcasted_iota(I32, (blocks, LANES), 1)
    live = row < live_buf[...]
    slots, ranks = slot_buf[...], rank_buf[...]
    live_jac[...] = jnp.where(live, jac_buf[...], 0.0)
    hi_of[...] = jnp.where(live, lax.shift_right_logical(slots, 7), 99)
    lo_of[...] = slots & (LANES - 1)
    lo_f[...] = (slots & (LANES - 1)).astype(F32)
    mark[...] = jnp.where(ranks == 3, 2.0**28, jnp.where(ranks == 2, 2.0**14, jnp.where(ranks == 1, 1.0, 0.0)))
    rank_f[...] = ranks.astype(F32)
    face_f[...] = encoded(face_buf[...])
    area = fold_rows(live_jac[...], jnp.add)[:1]
    area_total = jnp.sum(area, axis=1, keepdims=True) * total_weight

    whole_weight = jnp.broadcast_to(total_weight, (8, LANES))
    sixteen = lax.broadcasted_iota(I32, (16, LANES), 0)
    lo_ids = lax.broadcasted_iota(I32, (LANES, LANES), 0).astype(F32).astype(BF16)
    sums = jnp.zeros((64, LANES), F32)
    for c in range(PARTS):
        for copy in load(c):
            copy.wait()

    def project(c, width, count):
        part = pl.ds(c * width, width)
        data = jnp.concatenate([sec_buf[:, part], mst_buf[:, part]], axis=0)
        return jnp.dot(table[:count], data, preferred_element_type=F32)

    ahead = project(0, CHUNK, P_SIZE + 8)
    for c in range(chunks):
        found = ahead
        if c + 1 < chunks:
            ahead = project(c + 1, CHUNK, P_SIZE + 8)
        splits, marks = [], []
        for j in range(per):
            i = c * per + j
            at = slice(j * LANES, (j + 1) * LANES)
            offset = off_buf[pl.ds(i, 8, stride=0), :]
            row_pen = -(fold_rows(found[:P_SIZE, at], jnp.minimum) + offset)
            linear = fold_rows(found[P_SIZE : P_SIZE + 8, at], jnp.add)
            row_gap = jac_buf[pl.ds(i, 8, stride=0), :] * (linear + offset * whole_weight)
            member = hi_of[pl.ds(i, 16, stride=0), :] == sixteen
            pen_by[i] = jnp.where(member, jnp.concatenate([row_pen, row_pen], axis=0), LOWEST_FILL)
            terms = [jnp.concatenate([p, p], axis=0) for p in pieces(row_gap)]
            terms.append(mark[pl.ds(i, 16, stride=0), :])
            splits.append(jnp.concatenate([jnp.where(member, p, 0.0) for p in terms], axis=0).astype(BF16))
            lo = lo_f[pl.ds(i, 16, stride=0), :].astype(BF16)
            same = lo_ids.reshape(LANES // 16, 16, LANES) == lo[None]
            marks.append(jnp.where(same, jnp.bfloat16(1), jnp.bfloat16(0)).reshape(LANES, LANES))
            one_hot[:, pl.ds(i * LANES, LANES)] = marks[-1]
        sums = sums + lax.dot_general(
            jnp.concatenate(splits, axis=1), jnp.concatenate(marks, axis=1), (((1,), (1,)), ((), ())),
            preferred_element_type=F32,
        )
    seg_gap = sums[:16] + sums[16:32] + sums[32:48]
    code = sums[48:]
    best_rank = jnp.where(code >= 2.0**28, 3.0, jnp.where(code >= 2.0**14, 2.0, jnp.where(code >= 1.0, 1.0, 0.0)))
    gap_total = jnp.sum(jnp.sum(seg_gap, axis=0, keepdims=True), axis=1, keepdims=True)
    first_lane = lax.broadcasted_iota(I32, (1, LANES), 1) == 0
    plane_box[spot] = jnp.where(first_lane, gap_total, area_total)

    def plane_copy(k):
        return pltpu.make_async_remote_copy(
            src_ref=plane_box.at[spot], dst_ref=plane_box.at[spot],
            send_sem=plane_sem.at[0, k], recv_sem=plane_sem.at[1, k],
            device_id=plane_device(k), device_id_type=MESH,
        )

    def layer_copy(k):
        return pltpu.make_async_remote_copy(
            src_ref=layer_box.at[layer], dst_ref=layer_box.at[layer],
            send_sem=layer_sem.at[0, k], recv_sem=layer_sem.at[1, k],
            device_id=layer_device(k), device_id_type=MESH,
        )

    def own_copy(j, box, k):
        return pltpu.make_async_remote_copy(
            src_ref=box.at[rep], dst_ref=box.at[rep],
            send_sem=own_sem.at[0, j, k], recv_sem=own_sem.at[1, j, k],
            device_id=(dom, (rep + k) & (REPS - 1)), device_id_type=MESH,
        )

    def spill_copy(j, source, box, k):
        return pltpu.make_async_remote_copy(
            src_ref=source, dst_ref=box.at[rep],
            send_sem=spill_sem.at[0, j, k], recv_sem=spill_sem.at[1, j, k],
            device_id=((dom + 1) & (DOMS - 1), (rep + k) & (REPS - 1)), device_id_type=MESH,
        )

    pl.semaphore_wait(barrier, GREETED)

    @pl.loop(1, PLANE)
    def _(k):
        plane_copy(k).start()

    def search(jobs, his, group):
        @pl.loop(0, LANES // (8 * group))
        def _(g):
            base = pl.multiple_of(g * (8 * group), 8 * group)
            ids = [eight + (base + 8 * q) for q in range(group)]

            def step(i, carry):
                lo = lo_of[pl.ds(i, 8, stride=0), :]
                masks = [lo == ids[q] for q in range(group)]
                found = []
                for source, op, fill, _ in jobs:
                    for h in his:
                        value = source[i, pl.ds(h, 8, stride=0), :]
                        for mask in masks:
                            found.append(op(carry[len(found)], jnp.where(mask, value, fill)))
                return found

            start = [jnp.full((8, LANES), fill, F32) for _, _, fill, _ in jobs for _ in range(len(his) * group)]
            values = iter(lax.fori_loop(0, blocks, step, start, unroll=16))
            for _, _, _, acc in jobs:
                for h in his:
                    for q in range(group):
                        acc[h, pl.ds(base + 8 * q, 8), :] = next(values)

    pen_job = (pen_by, jnp.maximum, LOWEST_FILL, acc_pen)
    face_job = (face_by, jnp.minimum, FACE_FILL, acc_face)
    own_his, spill_his = tuple(range(8)), (8, 9)

    for c in range(chunks):
        wanted = jnp.dot(
            best_rank.astype(BF16), one_hot[:, pl.ds(c * CHUNK, CHUNK)], preferred_element_type=F32
        )
        for j in range(per):
            i = c * per + j
            member = hi_of[pl.ds(i, 16, stride=0), :] == sixteen
            member = member & (wanted[:, j * LANES : (j + 1) * LANES] == rank_f[pl.ds(i, 16, stride=0), :])
            face_by[i] = jnp.where(member, face_f[pl.ds(i, 16, stride=0), :], FACE_FILL)

    seg_pen = {}

    def settle_pens(his, box):
        for at, h in enumerate(his):
            seg_pen[h] = fold_rows(acc_pen[h].T, jnp.maximum)[:1]
            box[0, at : at + 1, :] = seg_pen[h]
            box[1, at : at + 1, :] = seg_gap[h : h + 1]
            box[2, at : at + 1, :] = jnp.where(seg_pen[h] <= 0.5 * LOWEST_FILL, -1.0, best_rank[h : h + 1])

    def settle_faces(his, box):
        for at, h in enumerate(his):
            value = fold_rows(acc_face[h].T, jnp.minimum)[:1]
            box[at : at + 1, :] = jnp.where(seg_pen[h] <= 0.5 * LOWEST_FILL, FACE_LIMIT, decoded(value))

    search([pen_job, face_job], spill_his, 4)
    settle_pens(spill_his, spill_f)
    settle_faces(spill_his, spill_i)
    sent = [spill_copy(0, spill_f, got_f, k) for k in (2, 1, 3, 0)]
    sent += [spill_copy(1, spill_i, got_i, k) for k in (2, 1, 3, 0)]
    for copy in sent:
        copy.start()

    search([pen_job], own_his, 2)
    settle_pens(own_his, own_f.at[rep])
    middle = [own_copy(0, own_f, k) for k in (2, 1, 3)]
    for copy in middle:
        copy.start()

    @pl.loop(1, PLANE)
    def _(k):
        plane_copy(k).wait()

    layer_box[layer] = jnp.sum(plane_box[...], axis=0)

    @pl.loop(1, LAYERS)
    def _(k):
        layer_copy(k).start()

    search([face_job], own_his, 2)
    settle_faces(own_his, own_i.at[rep])
    later = [own_copy(1, own_i, k) for k in (2, 1, 3)]
    for copy in later:
        copy.start()
    sent += middle

    half = 256
    ns = ns_buf[...]
    turns_of = rows // half

    def push_of(c, found):
        pushes = []
        for j in range(half // LANES):
            i = c * (half // LANES) + j
            gap = found[:, j * LANES : (j + 1) * LANES].reshape(P_SIZE // 8, 8, LANES)
            gap = gap + off_buf[pl.ds(i, 8, stride=0), :][None]
            push = jnp.maximum(weight[...].reshape(P_SIZE // 8, 8, LANES) * gap, 0.0)
            push = push * live_jac[pl.ds(i, 8, stride=0), :][None]
            pushes.append(push.reshape(P_SIZE, LANES).astype(BF16))
        return jnp.concatenate(pushes, axis=1)

    ahead, ready = project(0, half, P_SIZE), None
    for c in range(turns_of + 1):
        now = ahead
        if c + 1 < turns_of:
            ahead = project(c + 1, half, P_SIZE)
        if ready is not None:
            force_out[:, pl.ds((c - 1) * half, half)] = jnp.dot(ns, ready, preferred_element_type=F32).astype(BF16)
        if c < turns_of:
            ready = push_of(c, now)

    for copy in sent + later:
        copy.wait()

    def part_of(box_f, box_i, k):
        return box_f[k, 0], box_f[k, 2], box_i[k], box_f[k, 1]

    total = part_of(own_f, own_i, 0)
    for k in range(1, REPS):
        total = combine(total, part_of(own_f, own_i, k))
    reach = part_of(got_f, got_i, 0)
    for k in range(1, REPS):
        reach = combine(reach, part_of(got_f, got_i, k))
    leading = combine([x[:2] for x in total], reach)
    for at, (pen, top, face, gap_sum) in ((slice(0, 2), leading), (slice(2, 8), [x[2:] for x in total])):
        empty = top < 0.0
        pen_out[at, :] = jnp.where(empty, 0.0, pen)
        face_out[at, :] = jnp.where(empty, -1, face)
        gap_out[at, :] = gap_sum

    @pl.loop(1, LAYERS)
    def _(k):
        layer_copy(k).wait()

    totals = jnp.sum(layer_box[...], axis=0)
    mean_out[...] = jnp.broadcast_to(totals[:, :1] / totals[:, 1:2], (1, LANES))


def write_out(*refs):
    count = (len(refs) - 1) // 2
    copies = [pltpu.make_async_copy(refs[k], refs[count + k], refs[-1].at[k]) for k in range(count)]
    for copy in copies:
        copy.start()
    for copy in copies:
        copy.wait()


def shards(ns, nm, sec, mst, off, qw, jac, slot, face, rank, live):
    rows = sec.shape[1]
    chunks, blocks = rows // CHUNK, rows // LANES
    vmem = pl.BlockSpec(memory_space=pltpu.VMEM)
    hbm = pl.BlockSpec(memory_space=pl.ANY)

    def dense(x):
        return x.reshape(blocks, LANES)

    shapes = [((K, rows), BF16), ((8, LANES), F32), ((8, LANES), I32), ((8, LANES), F32), ((1, LANES), F32)]
    results = pl.pallas_call(
        kernel,
        out_shape=[pltpu.VMEM(shape, kind) for shape, kind in shapes],
        in_specs=[hbm] * 11,
        out_specs=[vmem] * 5,
        scratch_shapes=[
            pltpu.VMEM((K, P_SIZE), BF16),
            pltpu.VMEM((K, P_SIZE), BF16),
            pltpu.VMEM((K, rows), BF16),
            pltpu.VMEM((K, rows), BF16),
            pltpu.VMEM((blocks, LANES), F32),
            pltpu.VMEM((1, P_SIZE), F32),
            pltpu.VMEM((blocks, LANES), F32),
            pltpu.VMEM((blocks, LANES), I32),
            pltpu.VMEM((blocks, LANES), I32),
            pltpu.VMEM((blocks, LANES), I32),
            pltpu.VMEM((1, 1), I32),
            pltpu.VMEM((P_SIZE + 16, LANES), BF16),
            pltpu.VMEM((P_SIZE, LANES), F32),
            pltpu.VMEM((blocks, LANES), F32),
            pltpu.VMEM((blocks, LANES), I32),
            pltpu.VMEM((blocks, LANES), I32),
            pltpu.VMEM((blocks, LANES), F32),
            pltpu.VMEM((blocks, LANES), F32),
            pltpu.VMEM((blocks, LANES), F32),
            pltpu.VMEM((blocks, LANES), F32),
            pltpu.VMEM((LANES, rows), BF16),
            pltpu.VMEM((blocks, 16, LANES), F32),
            pltpu.VMEM((blocks, 16, LANES), F32),
            pltpu.VMEM((HIS, LANES, LANES), F32),
            pltpu.VMEM((HIS, LANES, LANES), F32),
            pltpu.VMEM((PLANE, 1, LANES), F32),
            pltpu.VMEM((LAYERS, 1, LANES), F32),
            pltpu.VMEM((REPS, 3, 8, LANES), F32),
            pltpu.VMEM((REPS, 8, LANES), I32),
            pltpu.VMEM((3, 2, LANES), F32),
            pltpu.VMEM((2, LANES), I32),
            pltpu.VMEM((REPS, 3, 2, LANES), F32),
            pltpu.VMEM((REPS, 2, LANES), I32),
            pltpu.SemaphoreType.DMA((2 * PARTS + 9,)),
            pltpu.SemaphoreType.DMA((2, PLANE)),
            pltpu.SemaphoreType.DMA((2, LAYERS)),
            pltpu.SemaphoreType.DMA((2, 2, REPS)),
            pltpu.SemaphoreType.DMA((2, 2, REPS)),
        ],
        compiler_params=pltpu.CompilerParams(
            vmem_limit_bytes=64_000_000, collective_id=0, has_side_effects=True
        ),
    )(ns, nm, sec, mst, dense(off), qw.reshape(1, -1), dense(jac), dense(slot), dense(face), dense(rank), live.reshape(1, 1))
    force, pen, face, gap, mean = pl.pallas_call(
        write_out,
        out_shape=[jax.ShapeDtypeStruct(shape, kind) for shape, kind in shapes],
        in_specs=[vmem] * 5,
        out_specs=[hbm] * 5,
        scratch_shapes=[pltpu.SemaphoreType.DMA((5,))],
        compiler_params=pltpu.CompilerParams(vmem_limit_bytes=1 << 20),
    )(*results)
    return force, pen.reshape(-1), face.reshape(-1), gap.reshape(-1), mean[0, 0]


def solution(mesh):
    both = P(("dom", "rep"))
    return jax.shard_map(
        shards,
        mesh=mesh,
        in_specs=(P(), P(), P(None, ("dom", "rep")), P(None, ("dom", "rep")), both, P()) + (both,) * 5,
        out_specs=(P(None, ("dom", "rep")), P("dom"), P("dom"), P("dom"), P()),
        check_vma=False,
    )
```

```python
import jax
import jax.numpy as jnp
from jax import lax
from jax.experimental import pallas as pl
from jax.experimental.pallas import tpu as pltpu
from jax.sharding import PartitionSpec as P

P_SIZE = 256
K = 64
LANES = 128
HIS = 10
PENALTY = 400.0
LOWEST_FILL = -1e30
FACE_LIMIT = 1073741824
FACE_FILL = 3e38
LOW_BITS = 1 << 23
CHUNK = 1024
PARTS = 2
F32 = jnp.float32
I32 = jnp.int32
BF16 = jnp.bfloat16
MESH = pl.DeviceIdType.MESH
DOMS = 64
REPS = 4
PLANE_DOMS = 8
PLANE = PLANE_DOMS * REPS
LAYERS = DOMS // PLANE_DOMS
GREETED = PLANE - 1 + LAYERS - 1 + REPS


def pieces(x):
    high = x.astype(BF16)
    rest = x - high.astype(F32)
    mid = rest.astype(BF16)
    low = (rest - mid.astype(F32)).astype(BF16)
    return high.astype(F32), mid.astype(F32), low.astype(F32)


def fold_rows(x, op):
    while x.shape[0] > 8:
        half = x.shape[0] // 2
        x = op(x[:half], x[half:])
    for shift in (4, 2, 1):
        x = op(x, pltpu.roll(x, shift, 0))
    return x


def encoded(face):
    scale = jnp.full(face.shape, 2.0**-87, F32)
    for t in range(7):
        scale = jnp.where((face & (LOW_BITS << t)) != 0, scale * 2.0 ** (1 << t), scale)
    return ((face & (LOW_BITS - 1)) + LOW_BITS).astype(F32) * scale


def decoded(value):
    top = jnp.zeros(value.shape, I32)
    for t in range(6, -1, -1):
        above = value >= 2.0 ** ((1 << t) - 64)
        value = jnp.where(above, value * 2.0 ** -(1 << t), value)
        top = jnp.where(above, top + (LOW_BITS << t), top)
    return (value * 2.0**87).astype(I32) - LOW_BITS + top


def combine(earlier, latter):
    prefer = (latter[1] > earlier[1]) | (latter[1] == earlier[1]) & (latter[2] < earlier[2])
    return (
        jnp.maximum(earlier[0], latter[0]),
        jnp.where(prefer, latter[1], earlier[1]),
        jnp.where(prefer, latter[2], earlier[2]),
        earlier[3] + latter[3],
    )


def kernel(
    ns_hbm, nm_hbm, sec_hbm, mst_hbm, off_hbm, qw_hbm, jac_hbm, slot_hbm, face_hbm, rank_hbm, live_hbm,
    force_out, pen_out, face_out, gap_out, mean_out,
    ns_buf, nm_buf, sec_buf, mst_buf, off_buf, qw_buf, jac_buf, slot_buf, face_buf, rank_buf, live_buf,
    table, weight, live_jac, hi_of, lo_of, lo_f, mark, rank_f, face_f, one_hot, pen_by, face_by, acc_pen, acc_face,
    plane_box, layer_box, own_f, own_i, spill_f, spill_i, got_f, got_i,
    in_sem, plane_sem, layer_sem, own_sem, spill_sem,
):
    rows = sec_hbm.shape[1]
    chunks = rows // CHUNK
    per = CHUNK // LANES
    dom, rep = lax.axis_index("dom"), lax.axis_index("rep")
    layer, spot = dom >> 3, (dom & 7) * REPS + rep

    def plane_device(k):
        other = (spot + k) & (PLANE - 1)
        return layer * PLANE_DOMS + (other >> 2), other & 3

    def layer_device(k):
        return ((layer + k) & (LAYERS - 1)) * PLANE_DOMS + (dom & 7), rep

    barrier = pltpu.get_barrier_semaphore()

    def greet(device):
        pl.semaphore_signal(barrier, inc=1, device_id=device, device_id_type=MESH)

    def load(c):
        part = pl.ds(c * (rows // PARTS), rows // PARTS)
        return (
            pltpu.make_async_copy(sec_hbm.at[:, part], sec_buf.at[:, part], in_sem.at[c]),
            pltpu.make_async_copy(mst_hbm.at[:, part], mst_buf.at[:, part], in_sem.at[PARTS + c]),
        )

    whole = (
        (ns_hbm, ns_buf), (nm_hbm, nm_buf), (qw_hbm, qw_buf), (live_hbm, live_buf), (jac_hbm, jac_buf),
        (slot_hbm, slot_buf), (face_hbm, face_buf), (rank_hbm, rank_buf), (off_hbm, off_buf),
    )
    singles = [pltpu.make_async_copy(a, b, in_sem.at[2 * PARTS + k]) for k, (a, b) in enumerate(whole)]
    @pl.loop(1, LAYERS)
    def _(k):
        greet(layer_device(k))

    for copy in singles:
        copy.start()
    for c in range(PARTS):
        for copy in load(c):
            copy.start()

    @pl.loop(1, PLANE)
    def _(k):
        greet(plane_device(k))

    @pl.loop(0, REPS)
    def _(k):
        greet(((dom + DOMS - 1) & (DOMS - 1), k))

    for copy in singles[:3]:
        copy.wait()
    ns = ns_buf[...]
    both = jnp.concatenate([ns.astype(F32), -nm_buf[...].astype(F32)], axis=0).T
    column = jnp.broadcast_to(qw_buf[...], (LANES, P_SIZE)).T
    weight[...] = column * (-PENALTY)
    total_weight = jnp.sum(qw_buf[...], axis=1, keepdims=True)
    coefficient = jnp.sum(both * column, axis=0, keepdims=True)
    high, mid, low = pieces(coefficient)
    eight = lax.broadcasted_iota(I32, (8, LANES), 0)
    extra = jnp.where(eight == 0, high, jnp.where(eight == 1, mid, jnp.where(eight == 2, low, 0.0)))
    table[...] = jnp.concatenate([both, extra, jnp.zeros_like(extra)], axis=0).astype(BF16)

    for copy in singles[3:]:
        copy.wait()
    blocks = rows // LANES
    row = lax.broadcasted_iota(I32, (blocks, LANES), 0) * LANES + lax.broadcasted_iota(I32, (blocks, LANES), 1)
    live = row < live_buf[...]
    slots, ranks = slot_buf[...], rank_buf[...]
    live_jac[...] = jnp.where(live, jac_buf[...], 0.0)
    hi_of[...] = jnp.where(live, lax.shift_right_logical(slots, 7), 99)
    lo_of[...] = slots & (LANES - 1)
    lo_f[...] = (slots & (LANES - 1)).astype(F32)
    mark[...] = jnp.where(ranks == 3, 2.0**28, jnp.where(ranks == 2, 2.0**14, jnp.where(ranks == 1, 1.0, 0.0)))
    rank_f[...] = ranks.astype(F32)
    face_f[...] = encoded(face_buf[...])
    area = fold_rows(live_jac[...], jnp.add)[:1]
    area_total = jnp.sum(area, axis=1, keepdims=True) * total_weight

    whole_weight = jnp.broadcast_to(total_weight, (8, LANES))
    sixteen = lax.broadcasted_iota(I32, (16, LANES), 0)
    lo_ids = lax.broadcasted_iota(I32, (LANES, LANES), 0).astype(F32).astype(BF16)
    sums = jnp.zeros((64, LANES), F32)
    live_gap = jnp.zeros((8, LANES), F32)
    for c in range(PARTS):
        for copy in load(c):
            copy.wait()

    def project(c, width, count):
        part = pl.ds(c * width, width)
        data = jnp.concatenate([sec_buf[:, part], mst_buf[:, part]], axis=0)
        return jnp.dot(table[:count], data, preferred_element_type=F32)

    ahead = project(0, CHUNK, P_SIZE + 8)
    for c in range(chunks):
        found = ahead
        if c + 1 < chunks:
            ahead = project(c + 1, CHUNK, P_SIZE + 8)
        splits, marks = [], []
        for j in range(per):
            i = c * per + j
            at = slice(j * LANES, (j + 1) * LANES)
            offset = off_buf[pl.ds(i, 8, stride=0), :]
            row_pen = -(fold_rows(found[:P_SIZE, at], jnp.minimum) + offset)
            linear = fold_rows(found[P_SIZE : P_SIZE + 8, at], jnp.add)
            linear = linear + offset * whole_weight
            row_gap = jac_buf[pl.ds(i, 8, stride=0), :] * linear
            live_gap = live_gap + live_jac[pl.ds(i, 8, stride=0), :] * linear
            member = hi_of[pl.ds(i, 16, stride=0), :] == sixteen
            pen_by[i] = jnp.where(member, jnp.concatenate([row_pen, row_pen], axis=0), LOWEST_FILL)
            terms = [jnp.concatenate([p, p], axis=0) for p in pieces(row_gap)]
            terms.append(mark[pl.ds(i, 16, stride=0), :])
            splits.append(jnp.concatenate([jnp.where(member, p, 0.0) for p in terms], axis=0).astype(BF16))
            lo = lo_f[pl.ds(i, 16, stride=0), :].astype(BF16)
            same = lo_ids.reshape(LANES // 16, 16, LANES) == lo[None]
            marks.append(jnp.where(same, jnp.bfloat16(1), jnp.bfloat16(0)).reshape(LANES, LANES))
            one_hot[:, pl.ds(i * LANES, LANES)] = marks[-1]
        sums = sums + lax.dot_general(
            jnp.concatenate(splits, axis=1), jnp.concatenate(marks, axis=1), (((1,), (1,)), ((), ())),
            preferred_element_type=F32,
        )
    seg_gap = sums[:16] + sums[16:32] + sums[32:48]
    code = sums[48:]
    best_rank = jnp.where(code >= 2.0**28, 3.0, jnp.where(code >= 2.0**14, 2.0, jnp.where(code >= 1.0, 1.0, 0.0)))
    gap_total = jnp.sum(live_gap[:1], axis=1, keepdims=True)
    first_lane = lax.broadcasted_iota(I32, (1, LANES), 1) == 0
    plane_box[spot] = jnp.where(first_lane, gap_total, area_total)

    def plane_copy(k):
        return pltpu.make_async_remote_copy(
            src_ref=plane_box.at[spot], dst_ref=plane_box.at[spot],
            send_sem=plane_sem.at[0, k], recv_sem=plane_sem.at[1, k],
            device_id=plane_device(k), device_id_type=MESH,
        )

    def layer_copy(k):
        return pltpu.make_async_remote_copy(
            src_ref=layer_box.at[layer], dst_ref=layer_box.at[layer],
            send_sem=layer_sem.at[0, k], recv_sem=layer_sem.at[1, k],
            device_id=layer_device(k), device_id_type=MESH,
        )

    def own_copy(j, box, k):
        return pltpu.make_async_remote_copy(
            src_ref=box.at[rep], dst_ref=box.at[rep],
            send_sem=own_sem.at[0, j, k], recv_sem=own_sem.at[1, j, k],
            device_id=(dom, (rep + k) & (REPS - 1)), device_id_type=MESH,
        )

    def spill_copy(j, source, box, k):
        return pltpu.make_async_remote_copy(
            src_ref=source, dst_ref=box.at[rep],
            send_sem=spill_sem.at[0, j, k], recv_sem=spill_sem.at[1, j, k],
            device_id=((dom + 1) & (DOMS - 1), (rep + k) & (REPS - 1)), device_id_type=MESH,
        )

    pl.semaphore_wait(barrier, GREETED)

    @pl.loop(1, PLANE)
    def _(k):
        plane_copy(k).start()

    def search(jobs, his, group, first=0, last=None):
        @pl.loop(first, LANES // (8 * group) if last is None else last)
        def _(g):
            base = pl.multiple_of(g * (8 * group), 8 * group)
            ids = [eight + (base + 8 * q) for q in range(group)]

            def step(i, carry):
                lo = lo_of[pl.ds(i, 8, stride=0), :]
                masks = [lo == ids[q] for q in range(group)]
                found = []
                for source, op, fill, _ in jobs:
                    for h in his:
                        value = source[i, pl.ds(h, 8, stride=0), :]
                        for mask in masks:
                            found.append(op(carry[len(found)], jnp.where(mask, value, fill)))
                return found

            start = [jnp.full((8, LANES), fill, F32) for _, _, fill, _ in jobs for _ in range(len(his) * group)]
            values = iter(lax.fori_loop(0, blocks, step, start, unroll=16))
            for _, _, _, acc in jobs:
                for h in his:
                    for q in range(group):
                        acc[h, pl.ds(base + 8 * q, 8), :] = next(values)

    pen_job = (pen_by, jnp.maximum, LOWEST_FILL, acc_pen)
    face_job = (face_by, jnp.minimum, FACE_FILL, acc_face)
    own_his, spill_his = tuple(range(8)), (8, 9)

    for c in range(chunks):
        wanted = jnp.dot(
            best_rank.astype(BF16), one_hot[:, pl.ds(c * CHUNK, CHUNK)], preferred_element_type=F32
        )
        for j in range(per):
            i = c * per + j
            member = hi_of[pl.ds(i, 16, stride=0), :] == sixteen
            member = member & (wanted[:, j * LANES : (j + 1) * LANES] == rank_f[pl.ds(i, 16, stride=0), :])
            face_by[i] = jnp.where(member, face_f[pl.ds(i, 16, stride=0), :], FACE_FILL)

    seg_pen = {}

    def settle_pens(his, box):
        for at, h in enumerate(his):
            seg_pen[h] = fold_rows(acc_pen[h].T, jnp.maximum)[:1]
            box[0, at : at + 1, :] = seg_pen[h]
            box[1, at : at + 1, :] = seg_gap[h : h + 1]
            box[2, at : at + 1, :] = jnp.where(seg_pen[h] <= 0.5 * LOWEST_FILL, -1.0, best_rank[h : h + 1])

    def settle_faces(his, box):
        for at, h in enumerate(his):
            value = fold_rows(acc_face[h].T, jnp.minimum)[:1]
            box[at : at + 1, :] = jnp.where(seg_pen[h] <= 0.5 * LOWEST_FILL, FACE_LIMIT, decoded(value))

    search([pen_job, face_job], spill_his, 4)
    settle_pens(spill_his, spill_f)
    settle_faces(spill_his, spill_i)
    sent = [spill_copy(0, spill_f, got_f, k) for k in (2, 1, 3, 0)]
    sent += [spill_copy(1, spill_i, got_i, k) for k in (2, 1, 3, 0)]
    for copy in sent:
        copy.start()

    search([pen_job], own_his, 2)
    settle_pens(own_his, own_f.at[rep])
    middle = [own_copy(0, own_f, k) for k in (2, 1, 3)]
    for copy in middle:
        copy.start()

    search([face_job], own_his, 2, 0, 1)

    @pl.loop(1, PLANE)
    def _(k):
        plane_copy(k).wait()

    layer_box[layer] = jnp.sum(plane_box[...], axis=0)

    @pl.loop(1, LAYERS)
    def _(k):
        layer_copy(k).start()

    search([face_job], own_his, 2, 1)
    settle_faces(own_his, own_i.at[rep])
    later = [own_copy(1, own_i, k) for k in (2, 1, 3)]
    for copy in later:
        copy.start()
    sent += middle

    half = 256
    ns = ns_buf[...]
    turns_of = rows // half

    def push_of(c, found):
        pushes = []
        for j in range(half // LANES):
            i = c * (half // LANES) + j
            gap = found[:, j * LANES : (j + 1) * LANES].reshape(P_SIZE // 8, 8, LANES)
            gap = gap + off_buf[pl.ds(i, 8, stride=0), :][None]
            push = jnp.maximum(weight[...].reshape(P_SIZE // 8, 8, LANES) * gap, 0.0)
            push = push * live_jac[pl.ds(i, 8, stride=0), :][None]
            pushes.append(push.reshape(P_SIZE, LANES).astype(BF16))
        return jnp.concatenate(pushes, axis=1)

    ahead, ready = project(0, half, P_SIZE), None
    for c in range(turns_of + 1):
        now = ahead
        if c + 1 < turns_of:
            ahead = project(c + 1, half, P_SIZE)
        if ready is not None:
            force_out[:, pl.ds((c - 1) * half, half)] = jnp.dot(ns, ready, preferred_element_type=F32).astype(BF16)
        if c < turns_of:
            ready = push_of(c, now)

    for copy in sent + later:
        copy.wait()

    def part_of(box_f, box_i, k):
        return box_f[k, 0], box_f[k, 2], box_i[k], box_f[k, 1]

    total = part_of(own_f, own_i, 0)
    for k in range(1, REPS):
        total = combine(total, part_of(own_f, own_i, k))
    reach = part_of(got_f, got_i, 0)
    for k in range(1, REPS):
        reach = combine(reach, part_of(got_f, got_i, k))
    leading = combine([x[:2] for x in total], reach)
    for at, (pen, top, face, gap_sum) in ((slice(0, 2), leading), (slice(2, 8), [x[2:] for x in total])):
        empty = top < 0.0
        pen_out[at, :] = jnp.where(empty, 0.0, pen)
        face_out[at, :] = jnp.where(empty, -1, face)
        gap_out[at, :] = gap_sum

    @pl.loop(1, LAYERS)
    def _(k):
        layer_copy(k).wait()

    totals = jnp.sum(layer_box[...], axis=0)
    mean_out[...] = jnp.broadcast_to(totals[:, :1] / totals[:, 1:2], (1, LANES))


def write_out(*refs):
    count = (len(refs) - 1) // 2
    copies = [pltpu.make_async_copy(refs[k], refs[count + k], refs[-1].at[k]) for k in range(count)]
    for copy in copies:
        copy.start()
    for copy in copies:
        copy.wait()


def shards(ns, nm, sec, mst, off, qw, jac, slot, face, rank, live):
    rows = sec.shape[1]
    chunks, blocks = rows // CHUNK, rows // LANES
    vmem = pl.BlockSpec(memory_space=pltpu.VMEM)
    hbm = pl.BlockSpec(memory_space=pl.ANY)

    def dense(x):
        return x.reshape(blocks, LANES)

    shapes = [((K, rows), BF16), ((8, LANES), F32), ((8, LANES), I32), ((8, LANES), F32), ((1, LANES), F32)]
    results = pl.pallas_call(
        kernel,
        out_shape=[pltpu.VMEM(shape, kind) for shape, kind in shapes],
        in_specs=[hbm] * 11,
        out_specs=[vmem] * 5,
        scratch_shapes=[
            pltpu.VMEM((K, P_SIZE), BF16),
            pltpu.VMEM((K, P_SIZE), BF16),
            pltpu.VMEM((K, rows), BF16),
            pltpu.VMEM((K, rows), BF16),
            pltpu.VMEM((blocks, LANES), F32),
            pltpu.VMEM((1, P_SIZE), F32),
            pltpu.VMEM((blocks, LANES), F32),
            pltpu.VMEM((blocks, LANES), I32),
            pltpu.VMEM((blocks, LANES), I32),
            pltpu.VMEM((blocks, LANES), I32),
            pltpu.VMEM((1, 1), I32),
            pltpu.VMEM((P_SIZE + 16, LANES), BF16),
            pltpu.VMEM((P_SIZE, LANES), F32),
            pltpu.VMEM((blocks, LANES), F32),
            pltpu.VMEM((blocks, LANES), I32),
            pltpu.VMEM((blocks, LANES), I32),
            pltpu.VMEM((blocks, LANES), F32),
            pltpu.VMEM((blocks, LANES), F32),
            pltpu.VMEM((blocks, LANES), F32),
            pltpu.VMEM((blocks, LANES), F32),
            pltpu.VMEM((LANES, rows), BF16),
            pltpu.VMEM((blocks, 16, LANES), F32),
            pltpu.VMEM((blocks, 16, LANES), F32),
            pltpu.VMEM((HIS, LANES, LANES), F32),
            pltpu.VMEM((HIS, LANES, LANES), F32),
            pltpu.VMEM((PLANE, 1, LANES), F32),
            pltpu.VMEM((LAYERS, 1, LANES), F32),
            pltpu.VMEM((REPS, 3, 8, LANES), F32),
            pltpu.VMEM((REPS, 8, LANES), I32),
            pltpu.VMEM((3, 2, LANES), F32),
            pltpu.VMEM((2, LANES), I32),
            pltpu.VMEM((REPS, 3, 2, LANES), F32),
            pltpu.VMEM((REPS, 2, LANES), I32),
            pltpu.SemaphoreType.DMA((2 * PARTS + 9,)),
            pltpu.SemaphoreType.DMA((2, PLANE)),
            pltpu.SemaphoreType.DMA((2, LAYERS)),
            pltpu.SemaphoreType.DMA((2, 2, REPS)),
            pltpu.SemaphoreType.DMA((2, 2, REPS)),
        ],
        compiler_params=pltpu.CompilerParams(
            vmem_limit_bytes=64_000_000, collective_id=0, has_side_effects=True
        ),
    )(ns, nm, sec, mst, dense(off), qw.reshape(1, -1), dense(jac), dense(slot), dense(face), dense(rank), live.reshape(1, 1))
    force, pen, face, gap, mean = pl.pallas_call(
        write_out,
        out_shape=[jax.ShapeDtypeStruct(shape, kind) for shape, kind in shapes],
        in_specs=[vmem] * 5,
        out_specs=[hbm] * 5,
        scratch_shapes=[pltpu.SemaphoreType.DMA((5,))],
        compiler_params=pltpu.CompilerParams(vmem_limit_bytes=1 << 20),
    )(*results)
    return force, pen.reshape(-1), face.reshape(-1), gap.reshape(-1), mean[0, 0]


def solution(mesh):
    both = P(("dom", "rep"))
    return jax.shard_map(
        shards,
        mesh=mesh,
        in_specs=(P(), P(), P(None, ("dom", "rep")), P(None, ("dom", "rep")), both, P()) + (both,) * 5,
        out_specs=(P(None, ("dom", "rep")), P("dom"), P("dom"), P("dom"), P()),
        check_vma=False,
    )
```

```python
import jax
import jax.numpy as jnp
from jax import lax
from jax.experimental import pallas as pl
from jax.experimental.pallas import tpu as pltpu
from jax.sharding import PartitionSpec as P

P_SIZE = 256
K = 64
LANES = 128
HIS = 10
PENALTY = 400.0
LOWEST_FILL = -1e30
FACE_LIMIT = 1073741824
FACE_FILL = 3e38
LOW_BITS = 1 << 23
CHUNK = 1024
PARTS = 2
F32 = jnp.float32
I32 = jnp.int32
BF16 = jnp.bfloat16
MESH = pl.DeviceIdType.MESH
DOMS = 64
REPS = 4
PLANE_DOMS = 8
PLANE = PLANE_DOMS * REPS
LAYERS = DOMS // PLANE_DOMS
GREETED = PLANE - 1 + LAYERS - 1 + REPS


def pieces(x):
    high = x.astype(BF16)
    rest = x - high.astype(F32)
    mid = rest.astype(BF16)
    low = (rest - mid.astype(F32)).astype(BF16)
    return high.astype(F32), mid.astype(F32), low.astype(F32)


def fold_rows(x, op):
    while x.shape[0] > 8:
        half = x.shape[0] // 2
        x = op(x[:half], x[half:])
    for shift in (4, 2, 1):
        x = op(x, pltpu.roll(x, shift, 0))
    return x


def encoded(face):
    scale = jnp.full(face.shape, 2.0**-87, F32)
    for t in range(7):
        scale = jnp.where((face & (LOW_BITS << t)) != 0, scale * 2.0 ** (1 << t), scale)
    return ((face & (LOW_BITS - 1)) + LOW_BITS).astype(F32) * scale


def decoded(value):
    top = jnp.zeros(value.shape, I32)
    for t in range(6, -1, -1):
        above = value >= 2.0 ** ((1 << t) - 64)
        value = jnp.where(above, value * 2.0 ** -(1 << t), value)
        top = jnp.where(above, top + (LOW_BITS << t), top)
    return (value * 2.0**87).astype(I32) - LOW_BITS + top


def combine(earlier, latter):
    prefer = (latter[1] > earlier[1]) | (latter[1] == earlier[1]) & (latter[2] < earlier[2])
    return (
        jnp.maximum(earlier[0], latter[0]),
        jnp.where(prefer, latter[1], earlier[1]),
        jnp.where(prefer, latter[2], earlier[2]),
        earlier[3] + latter[3],
    )


def kernel(
    ns_hbm, nm_hbm, sec_hbm, mst_hbm, off_hbm, qw_hbm, jac_hbm, slot_hbm, face_hbm, rank_hbm, live_hbm,
    force_out, pen_out, face_out, gap_out, mean_out,
    ns_buf, nm_buf, sec_buf, mst_buf, off_buf, qw_buf, jac_buf, slot_buf, face_buf, rank_buf, live_buf,
    table, weight, live_jac, hi_of, lo_of, lo_f, mark, rank_f, face_f, one_hot, pen_by, face_by, acc_pen, acc_face,
    plane_box, layer_box, own_f, own_i, spill_f, spill_i, got_f, got_i,
    in_sem, plane_sem, layer_sem, own_sem, spill_sem,
):
    rows = sec_hbm.shape[1]
    chunks = rows // CHUNK
    per = CHUNK // LANES
    dom, rep = lax.axis_index("dom"), lax.axis_index("rep")
    layer, spot = dom >> 3, (dom & 7) * REPS + rep

    def plane_device(k):
        other = (spot + k) & (PLANE - 1)
        return layer * PLANE_DOMS + (other >> 2), other & 3

    def layer_device(k):
        return ((layer + k) & (LAYERS - 1)) * PLANE_DOMS + (dom & 7), rep

    barrier = pltpu.get_barrier_semaphore()

    def greet(device):
        pl.semaphore_signal(barrier, inc=1, device_id=device, device_id_type=MESH)

    def load(c):
        part = pl.ds(c * (rows // PARTS), rows // PARTS)
        return (
            pltpu.make_async_copy(sec_hbm.at[:, part], sec_buf.at[:, part], in_sem.at[c]),
            pltpu.make_async_copy(mst_hbm.at[:, part], mst_buf.at[:, part], in_sem.at[PARTS + c]),
        )

    whole = (
        (ns_hbm, ns_buf), (nm_hbm, nm_buf), (qw_hbm, qw_buf), (live_hbm, live_buf), (jac_hbm, jac_buf),
        (slot_hbm, slot_buf), (face_hbm, face_buf), (rank_hbm, rank_buf), (off_hbm, off_buf),
    )
    singles = [pltpu.make_async_copy(a, b, in_sem.at[2 * PARTS + k]) for k, (a, b) in enumerate(whole)]
    @pl.loop(1, LAYERS)
    def _(k):
        greet(layer_device(k))

    for copy in singles:
        copy.start()
    for c in range(PARTS):
        for copy in load(c):
            copy.start()

    @pl.loop(1, PLANE)
    def _(k):
        greet(plane_device(k))

    @pl.loop(0, REPS)
    def _(k):
        greet(((dom + DOMS - 1) & (DOMS - 1), k))

    for copy in singles[:3]:
        copy.wait()
    ns = ns_buf[...]
    both = jnp.concatenate([ns.astype(F32), -nm_buf[...].astype(F32)], axis=0).T
    column = jnp.broadcast_to(qw_buf[...], (LANES, P_SIZE)).T
    weight[...] = column * (-PENALTY)
    total_weight = jnp.sum(qw_buf[...], axis=1, keepdims=True)
    coefficient = jnp.sum(both * column, axis=0, keepdims=True)
    high, mid, low = pieces(coefficient)
    eight = lax.broadcasted_iota(I32, (8, LANES), 0)
    extra = jnp.where(eight == 0, high, jnp.where(eight == 1, mid, jnp.where(eight == 2, low, 0.0)))
    table[...] = jnp.concatenate([both, extra, jnp.zeros_like(extra)], axis=0).astype(BF16)

    for copy in singles[3:]:
        copy.wait()
    blocks = rows // LANES
    row = lax.broadcasted_iota(I32, (blocks, LANES), 0) * LANES + lax.broadcasted_iota(I32, (blocks, LANES), 1)
    live = row < live_buf[...]
    slots, ranks = slot_buf[...], rank_buf[...]
    live_jac[...] = jnp.where(live, jac_buf[...], 0.0)
    hi_of[...] = jnp.where(live, lax.shift_right_logical(slots, 7), 99)
    lo_of[...] = slots & (LANES - 1)
    lo_f[...] = (slots & (LANES - 1)).astype(F32)
    mark[...] = jnp.where(ranks == 3, 2.0**28, jnp.where(ranks == 2, 2.0**14, jnp.where(ranks == 1, 1.0, 0.0)))
    rank_f[...] = ranks.astype(F32)
    face_f[...] = encoded(face_buf[...])
    area = fold_rows(live_jac[...], jnp.add)[:1]
    area_total = jnp.sum(area, axis=1, keepdims=True) * total_weight

    whole_weight = jnp.broadcast_to(total_weight, (8, LANES))
    sixteen = lax.broadcasted_iota(I32, (16, LANES), 0)
    lo_ids = lax.broadcasted_iota(I32, (LANES, LANES), 0).astype(F32).astype(BF16)
    sums = jnp.zeros((64, LANES), F32)
    live_gap = jnp.zeros((8, LANES), F32)
    for c in range(PARTS):
        for copy in load(c):
            copy.wait()

    def project(c, width, count):
        part = pl.ds(c * width, width)
        data = jnp.concatenate([sec_buf[:, part], mst_buf[:, part]], axis=0)
        return jnp.dot(table[:count], data, preferred_element_type=F32)

    ahead = project(0, CHUNK, P_SIZE + 8)
    for c in range(chunks):
        found = ahead
        if c + 1 < chunks:
            ahead = project(c + 1, CHUNK, P_SIZE + 8)
        splits, marks = [], []
        for j in range(per):
            i = c * per + j
            at = slice(j * LANES, (j + 1) * LANES)
            offset = off_buf[pl.ds(i, 8, stride=0), :]
            row_pen = -(fold_rows(found[:P_SIZE, at], jnp.minimum) + offset)
            linear = fold_rows(found[P_SIZE : P_SIZE + 8, at], jnp.add)
            linear = linear + offset * whole_weight
            row_gap = jac_buf[pl.ds(i, 8, stride=0), :] * linear
            live_gap = live_gap + live_jac[pl.ds(i, 8, stride=0), :] * linear
            member = hi_of[pl.ds(i, 16, stride=0), :] == sixteen
            pen_by[i] = jnp.where(member, jnp.concatenate([row_pen, row_pen], axis=0), LOWEST_FILL)
            terms = [jnp.concatenate([p, p], axis=0) for p in pieces(row_gap)]
            terms.append(mark[pl.ds(i, 16, stride=0), :])
            splits.append(jnp.concatenate([jnp.where(member, p, 0.0) for p in terms], axis=0).astype(BF16))
            lo = lo_f[pl.ds(i, 16, stride=0), :].astype(BF16)
            same = lo_ids.reshape(LANES // 16, 16, LANES) == lo[None]
            marks.append(jnp.where(same, jnp.bfloat16(1), jnp.bfloat16(0)).reshape(LANES, LANES))
            one_hot[:, pl.ds(i * LANES, LANES)] = marks[-1]
        sums = sums + lax.dot_general(
            jnp.concatenate(splits, axis=1), jnp.concatenate(marks, axis=1), (((1,), (1,)), ((), ())),
            preferred_element_type=F32,
        )
    seg_gap = sums[:16] + sums[16:32] + sums[32:48]
    code = sums[48:]
    best_rank = jnp.where(code >= 2.0**28, 3.0, jnp.where(code >= 2.0**14, 2.0, jnp.where(code >= 1.0, 1.0, 0.0)))
    gap_total = jnp.sum(live_gap[:1], axis=1, keepdims=True)
    first_lane = lax.broadcasted_iota(I32, (1, LANES), 1) == 0
    plane_box[spot] = jnp.where(first_lane, gap_total, area_total)

    def plane_copy(k):
        return pltpu.make_async_remote_copy(
            src_ref=plane_box.at[spot], dst_ref=plane_box.at[spot],
            send_sem=plane_sem.at[0, k], recv_sem=plane_sem.at[1, k],
            device_id=plane_device(k), device_id_type=MESH,
        )

    def layer_copy(k):
        return pltpu.make_async_remote_copy(
            src_ref=layer_box.at[layer], dst_ref=layer_box.at[layer],
            send_sem=layer_sem.at[0, k], recv_sem=layer_sem.at[1, k],
            device_id=layer_device(k), device_id_type=MESH,
        )

    def own_copy(j, box, k):
        return pltpu.make_async_remote_copy(
            src_ref=box.at[rep], dst_ref=box.at[rep],
            send_sem=own_sem.at[0, j, k], recv_sem=own_sem.at[1, j, k],
            device_id=(dom, (rep + k) & (REPS - 1)), device_id_type=MESH,
        )

    def spill_copy(j, source, box, k):
        return pltpu.make_async_remote_copy(
            src_ref=source, dst_ref=box.at[rep],
            send_sem=spill_sem.at[0, j, k], recv_sem=spill_sem.at[1, j, k],
            device_id=((dom + 1) & (DOMS - 1), (rep + k) & (REPS - 1)), device_id_type=MESH,
        )

    pl.semaphore_wait(barrier, GREETED)

    @pl.loop(1, PLANE)
    def _(k):
        plane_copy(k).start()

    def search(jobs, his, group, first=0, last=None):
        @pl.loop(first, LANES // (8 * group) if last is None else last)
        def _(g):
            base = pl.multiple_of(g * (8 * group), 8 * group)
            ids = [eight + (base + 8 * q) for q in range(group)]

            def step(i, carry):
                lo = lo_of[pl.ds(i, 8, stride=0), :]
                masks = [lo == ids[q] for q in range(group)]
                found = []
                for source, op, fill, _ in jobs:
                    for h in his:
                        value = source[i, pl.ds(h, 8, stride=0), :]
                        for mask in masks:
                            found.append(op(carry[len(found)], jnp.where(mask, value, fill)))
                return found

            start = [jnp.full((8, LANES), fill, F32) for _, _, fill, _ in jobs for _ in range(len(his) * group)]
            values = iter(lax.fori_loop(0, blocks, step, start, unroll=32))
            for _, _, _, acc in jobs:
                for h in his:
                    for q in range(group):
                        acc[h, pl.ds(base + 8 * q, 8), :] = next(values)

    pen_job = (pen_by, jnp.maximum, LOWEST_FILL, acc_pen)
    face_job = (face_by, jnp.minimum, FACE_FILL, acc_face)
    own_his, spill_his = tuple(range(8)), (8, 9)

    for c in range(chunks):
        wanted = jnp.dot(
            best_rank.astype(BF16), one_hot[:, pl.ds(c * CHUNK, CHUNK)], preferred_element_type=F32
        )
        for j in range(per):
            i = c * per + j
            member = hi_of[pl.ds(i, 16, stride=0), :] == sixteen
            member = member & (wanted[:, j * LANES : (j + 1) * LANES] == rank_f[pl.ds(i, 16, stride=0), :])
            face_by[i] = jnp.where(member, face_f[pl.ds(i, 16, stride=0), :], FACE_FILL)

    seg_pen = {}

    def settle_pens(his, box):
        for at, h in enumerate(his):
            seg_pen[h] = fold_rows(acc_pen[h].T, jnp.maximum)[:1]
            box[0, at : at + 1, :] = seg_pen[h]
            box[1, at : at + 1, :] = seg_gap[h : h + 1]
            box[2, at : at + 1, :] = jnp.where(seg_pen[h] <= 0.5 * LOWEST_FILL, -1.0, best_rank[h : h + 1])

    def settle_faces(his, box):
        for at, h in enumerate(his):
            value = fold_rows(acc_face[h].T, jnp.minimum)[:1]
            box[at : at + 1, :] = jnp.where(seg_pen[h] <= 0.5 * LOWEST_FILL, FACE_LIMIT, decoded(value))

    search([pen_job, face_job], spill_his, 4)
    settle_pens(spill_his, spill_f)
    settle_faces(spill_his, spill_i)
    sent = [spill_copy(0, spill_f, got_f, k) for k in (2, 1, 3, 0)]
    sent += [spill_copy(1, spill_i, got_i, k) for k in (2, 1, 3, 0)]
    for copy in sent:
        copy.start()

    search([pen_job], own_his, 2)
    settle_pens(own_his, own_f.at[rep])
    middle = [own_copy(0, own_f, k) for k in (2, 1, 3)]
    for copy in middle:
        copy.start()

    search([face_job], own_his, 2, 0, 1)

    @pl.loop(1, PLANE)
    def _(k):
        plane_copy(k).wait()

    layer_box[layer] = jnp.sum(plane_box[...], axis=0)

    @pl.loop(1, LAYERS)
    def _(k):
        layer_copy(k).start()

    search([face_job], own_his, 2, 1)
    settle_faces(own_his, own_i.at[rep])
    later = [own_copy(1, own_i, k) for k in (2, 1, 3)]
    for copy in later:
        copy.start()
    sent += middle

    half = 256
    ns = ns_buf[...]
    turns_of = rows // half

    def push_of(c, found):
        pushes = []
        for j in range(half // LANES):
            i = c * (half // LANES) + j
            gap = found[:, j * LANES : (j + 1) * LANES].reshape(P_SIZE // 8, 8, LANES)
            gap = gap + off_buf[pl.ds(i, 8, stride=0), :][None]
            push = jnp.maximum(weight[...].reshape(P_SIZE // 8, 8, LANES) * gap, 0.0)
            push = push * live_jac[pl.ds(i, 8, stride=0), :][None]
            pushes.append(push.reshape(P_SIZE, LANES).astype(BF16))
        return jnp.concatenate(pushes, axis=1)

    ahead, ready = project(0, half, P_SIZE), None
    for c in range(turns_of + 1):
        now = ahead
        if c + 1 < turns_of:
            ahead = project(c + 1, half, P_SIZE)
        if ready is not None:
            force_out[:, pl.ds((c - 1) * half, half)] = jnp.dot(ns, ready, preferred_element_type=F32).astype(BF16)
        if c < turns_of:
            ready = push_of(c, now)

    for copy in sent + later:
        copy.wait()

    def part_of(box_f, box_i, k):
        return box_f[k, 0], box_f[k, 2], box_i[k], box_f[k, 1]

    total = part_of(own_f, own_i, 0)
    for k in range(1, REPS):
        total = combine(total, part_of(own_f, own_i, k))
    reach = part_of(got_f, got_i, 0)
    for k in range(1, REPS):
        reach = combine(reach, part_of(got_f, got_i, k))
    leading = combine([x[:2] for x in total], reach)
    for at, (pen, top, face, gap_sum) in ((slice(0, 2), leading), (slice(2, 8), [x[2:] for x in total])):
        empty = top < 0.0
        pen_out[at, :] = jnp.where(empty, 0.0, pen)
        face_out[at, :] = jnp.where(empty, -1, face)
        gap_out[at, :] = gap_sum

    @pl.loop(1, LAYERS)
    def _(k):
        layer_copy(k).wait()

    totals = jnp.sum(layer_box[...], axis=0)
    mean_out[...] = jnp.broadcast_to(totals[:, :1] / totals[:, 1:2], (1, LANES))


def write_out(*refs):
    count = (len(refs) - 1) // 2
    copies = [pltpu.make_async_copy(refs[k], refs[count + k], refs[-1].at[k]) for k in range(count)]
    for copy in copies:
        copy.start()
    for copy in copies:
        copy.wait()


def shards(ns, nm, sec, mst, off, qw, jac, slot, face, rank, live):
    rows = sec.shape[1]
    chunks, blocks = rows // CHUNK, rows // LANES
    vmem = pl.BlockSpec(memory_space=pltpu.VMEM)
    hbm = pl.BlockSpec(memory_space=pl.ANY)

    def dense(x):
        return x.reshape(blocks, LANES)

    shapes = [((K, rows), BF16), ((8, LANES), F32), ((8, LANES), I32), ((8, LANES), F32), ((1, LANES), F32)]
    results = pl.pallas_call(
        kernel,
        out_shape=[pltpu.VMEM(shape, kind) for shape, kind in shapes],
        in_specs=[hbm] * 11,
        out_specs=[vmem] * 5,
        scratch_shapes=[
            pltpu.VMEM((K, P_SIZE), BF16),
            pltpu.VMEM((K, P_SIZE), BF16),
            pltpu.VMEM((K, rows), BF16),
            pltpu.VMEM((K, rows), BF16),
            pltpu.VMEM((blocks, LANES), F32),
            pltpu.VMEM((1, P_SIZE), F32),
            pltpu.VMEM((blocks, LANES), F32),
            pltpu.VMEM((blocks, LANES), I32),
            pltpu.VMEM((blocks, LANES), I32),
            pltpu.VMEM((blocks, LANES), I32),
            pltpu.VMEM((1, 1), I32),
            pltpu.VMEM((P_SIZE + 16, LANES), BF16),
            pltpu.VMEM((P_SIZE, LANES), F32),
            pltpu.VMEM((blocks, LANES), F32),
            pltpu.VMEM((blocks, LANES), I32),
            pltpu.VMEM((blocks, LANES), I32),
            pltpu.VMEM((blocks, LANES), F32),
            pltpu.VMEM((blocks, LANES), F32),
            pltpu.VMEM((blocks, LANES), F32),
            pltpu.VMEM((blocks, LANES), F32),
            pltpu.VMEM((LANES, rows), BF16),
            pltpu.VMEM((blocks, 16, LANES), F32),
            pltpu.VMEM((blocks, 16, LANES), F32),
            pltpu.VMEM((HIS, LANES, LANES), F32),
            pltpu.VMEM((HIS, LANES, LANES), F32),
            pltpu.VMEM((PLANE, 1, LANES), F32),
            pltpu.VMEM((LAYERS, 1, LANES), F32),
            pltpu.VMEM((REPS, 3, 8, LANES), F32),
            pltpu.VMEM((REPS, 8, LANES), I32),
            pltpu.VMEM((3, 2, LANES), F32),
            pltpu.VMEM((2, LANES), I32),
            pltpu.VMEM((REPS, 3, 2, LANES), F32),
            pltpu.VMEM((REPS, 2, LANES), I32),
            pltpu.SemaphoreType.DMA((2 * PARTS + 9,)),
            pltpu.SemaphoreType.DMA((2, PLANE)),
            pltpu.SemaphoreType.DMA((2, LAYERS)),
            pltpu.SemaphoreType.DMA((2, 2, REPS)),
            pltpu.SemaphoreType.DMA((2, 2, REPS)),
        ],
        compiler_params=pltpu.CompilerParams(
            vmem_limit_bytes=64_000_000, collective_id=0, has_side_effects=True
        ),
    )(ns, nm, sec, mst, dense(off), qw.reshape(1, -1), dense(jac), dense(slot), dense(face), dense(rank), live.reshape(1, 1))
    force, pen, face, gap, mean = pl.pallas_call(
        write_out,
        out_shape=[jax.ShapeDtypeStruct(shape, kind) for shape, kind in shapes],
        in_specs=[vmem] * 5,
        out_specs=[hbm] * 5,
        scratch_shapes=[pltpu.SemaphoreType.DMA((5,))],
        compiler_params=pltpu.CompilerParams(vmem_limit_bytes=1 << 20),
    )(*results)
    return force, pen.reshape(-1), face.reshape(-1), gap.reshape(-1), mean[0, 0]


def solution(mesh):
    both = P(("dom", "rep"))
    return jax.shard_map(
        shards,
        mesh=mesh,
        in_specs=(P(), P(), P(None, ("dom", "rep")), P(None, ("dom", "rep")), both, P()) + (both,) * 5,
        out_specs=(P(None, ("dom", "rep")), P("dom"), P("dom"), P("dom"), P()),
        check_vma=False,
    )
```
